16 devices in a mesh: rep: 2 (over y, z), dp: 8 (over x, core).
Axes of the slice: x: 4, y: 2, z: 1, core: 2. Of those that a mesh axis runs over, the one named last changes fastest.
The devices are a block of a 4x4x8 slice.
Arguments:
- x: bfloat16 [16, 2048, 512], P(('rep', 'dp')), parts along dimension 0
- dy: bfloat16 [16, 2048, 512], P(('rep', 'dp')), parts along dimension 0
- w_gate: bfloat16 [2, 512, 1664], replicated
- w_up: bfloat16 [2, 512, 1664], replicated
- w_down: bfloat16 [2, 1664, 512], replicated
- m_w_gate: float32 [2, 512, 1664], replicated
- m_w_up: float32 [2, 512, 1664], replicated
- m_w_down: float32 [2, 1664, 512], replicated
- v_w_gate: float32 [2, 512, 1664], replicated
- v_w_up: float32 [2, 512, 1664], replicated
- v_w_down: float32 [2, 1664, 512], replicated
Outputs:
- output 1: bfloat16 [4, 512, 1664], P('rep'), parts along dimension 0
- output 2: bfloat16 [4, 512, 1664], P('rep'), parts along dimension 0
- output 3: bfloat16 [4, 1664, 512], P('rep'), parts along dimension 0
- output 4: float32 [4, 512, 1664], P('rep'), parts along dimension 0
- output 5: float32 [4, 512, 1664], P('rep'), parts along dimension 0
- output 6: float32 [4, 1664, 512], P('rep'), parts along dimension 0
- output 7: float32 [4, 512, 1664], P('rep'), parts along dimension 0
- output 8: float32 [4, 512, 1664], P('rep'), parts along dimension 0
- output 9: float32 [4, 1664, 512], P('rep'), parts along dimension 0
There are 2 independent parts. The reference program is written for one: setup_inputs(seed, part) draws one part's arguments, and reference() takes and returns one part's arrays. A program takes and returns all parts, laid end to end along the dimension named above; an argument that names none is the same for every part.
All inputs are finite; a program needn't handle non-finite values.
Results may differ from the reference program's by a relative error of at most 0.0202.
Values are sent between devices in bfloat16 or wider.
A program may use at most 768 MiB of HBM per device.

```python
import jax
import jax.numpy as jnp
from jax import lax

SEQUENCES = 8
TOKENS = 2048
D = 512
FF = 1664
LAYERS = 2
NAMES = ("w_gate", "w_up", "w_down")
SHAPES = {"w_gate": (LAYERS, D, FF), "w_up": (LAYERS, D, FF), "w_down": (LAYERS, FF, D)}


def bump(key, n, height):
    away = (jnp.arange(n, dtype=jnp.int32) - jax.random.randint(key, (), 0, n, jnp.int32)) % n
    return jnp.where(away < n // 8, height, 1.0)


def together(key, own, strength):
    shared = jax.random.normal(key, own.shape[1:], jnp.float32)
    return (own + strength * shared) * lax.rsqrt(1 + strength * strength)


def setup_inputs(seed: int = 0, part: int = 0) -> dict:
    kx, kdy, ka, kb, kz, kf, kh, kl, *keys = jax.random.split(jax.random.key(seed), 8 + 3 * len(NAMES))
    kx, kdy, ka, kb = (jax.random.fold_in(k, part) for k in (kx, kdy, ka, kb))
    kw, km, kv = (keys[i::3] for i in range(3))
    shape = (SEQUENCES, TOKENS, D)
    much_x, much_dy = jax.random.uniform(kz, (2,), jnp.float32, 0.0, 1.0)
    loud = 2.0 ** jax.random.uniform(jax.random.fold_in(kz, 1), (), jnp.float32, -1.0, 2.0)
    layers = 2.0 ** jax.random.uniform(kl, (LAYERS, 1, 1), jnp.float32, -1.0, 1.0)
    x = together(ka, jax.random.normal(kx, shape, jnp.float32), much_x) * bump(kf, D, 4.0)
    dy = together(kb, jax.random.normal(kdy, shape, jnp.float32), much_dy)
    drawn = {"x": x.astype(jnp.bfloat16), "dy": (loud * dy * (SEQUENCES * TOKENS) ** -0.5).astype(jnp.bfloat16)}
    for key, name in zip(kw, NAMES, strict=True):
        w = jax.random.normal(key, SHAPES[name], jnp.float32) * SHAPES[name][1] ** -0.5
        drawn[name] = (w * {"w_gate": 1.0, "w_up": bump(kh, FF, 4.0), "w_down": layers}[name]).astype(jnp.bfloat16)
    for key, name in zip(km, NAMES, strict=True):
        drawn[f"m_{name}"] = 0.1 * jax.random.normal(key, SHAPES[name], jnp.float32)
    for key, name in zip(kv, NAMES, strict=True):
        drawn[f"v_{name}"] = jax.random.uniform(key, SHAPES[name], jnp.float32, 0.005, 0.015)
    return drawn


def matmul(a, w):
    return jnp.dot(a, w, preferred_element_type=jnp.float32).astype(jnp.bfloat16)


def normed(h):
    wide = h.astype(jnp.float32)
    scale = lax.rsqrt(jnp.mean(wide**2, -1, keepdims=True) + 1e-6)
    return (wide * scale).astype(jnp.bfloat16)


def layer(h, w):
    a = normed(h)
    gate = jnp.dot(a, w["w_gate"], preferred_element_type=jnp.float32)
    up = jnp.dot(a, w["w_up"], preferred_element_type=jnp.float32)
    return h + matmul((jax.nn.silu(gate) * up).astype(jnp.bfloat16), w["w_down"])


def adamw(w, m, v, g):
    m = 0.9 * m + 0.1 * g
    v = 0.95 * v + 0.05 * g * g
    step = m * lax.rsqrt(v + 1e-8) + 0.1 * w
    return (w - 0.02 * step).astype(jnp.bfloat16), m, v


def stack(weights, h):
    return lax.scan(lambda h, w: (layer(h, w), None), h, weights)[0]


def reference(x, dy, w_gate, w_up, w_down, m_w_gate, m_w_up, m_w_down, v_w_gate, v_w_up, v_w_down):
    weights = dict(zip(NAMES, (w_gate, w_up, w_down), strict=True))

    def take(so_far, sequence):
        h, by_y = sequence
        _, back = jax.vjp(lambda w: stack(w, h), weights)
        return jax.tree.map(lambda total, term: total + term.astype(jnp.float32), so_far, back(by_y)[0]), None

    none_yet = {name: jnp.zeros(w.shape, jnp.float32) for name, w in weights.items()}
    by_weights, _ = lax.scan(take, none_yet, (x, dy))
    gradients = [by_weights[name].astype(jnp.bfloat16).astype(jnp.float32) for name in NAMES]
    new = [
        adamw(w.astype(jnp.float32), m, v, g)
        for w, m, v, g in zip((w_gate, w_up, w_down), (m_w_gate, m_w_up, m_w_down), (v_w_gate, v_w_up, v_w_down), gradients, strict=True)
    ]
    return tuple(one[which] for which in range(3) for one in new)
```

```python
import jax
import jax.numpy as jnp
from jax import lax
from jax.experimental import pallas as pl
from jax.experimental.pallas import tpu as pltpu
from jax.sharding import PartitionSpec as P

ANY = pl.BlockSpec(memory_space=pl.ANY)
LANES = 128
BF16, F32 = jnp.bfloat16, jnp.float32
MESH = pl.DeviceIdType.MESH


def dot(a, b, dims=((1,), (0,))):
    return lax.dot_general(a, b, (dims, ((), ())), preferred_element_type=F32)


def dot_t(a, b):
    return dot(a, b, ((1,), (1,)))


def normed(h):
    wide = h.astype(F32)
    scale = lax.rsqrt(jnp.mean(wide * wide, -1, keepdims=True) + 1e-6)
    return (wide * scale).astype(BF16)


def interleaved(wg, wu, layer, to, sem):
    out = []
    for j in range(wg.shape[2] // LANES):
        for n, w in enumerate((wg, wu)):
            out.append(pltpu.make_async_copy(w.at[layer, :, pl.ds(j * LANES, LANES)], to.at[:, pl.ds((2 * j + n) * LANES, LANES)], sem))
    return out


def pairs(blocks):
    return [(at, min(2, blocks - at)) for at in range(0, blocks, 2)]


def backward_of_product(gate, up, dp):
    s = jax.nn.sigmoid(gate)
    silu = gate * s
    return silu, (dp * up * (s + silu * (1 - s))).astype(BF16), (dp * silu).astype(BF16)


def forward_kernel(x_ref, dy_ref, wg, wu, wd, a0_ref, a0t_ref, h1_ref, a1t_ref, mid0t_ref, mid1t_ref, dg_ref, du_ref, wgu, wdv, mid0, sem):
    blocks = wg.shape[2] // LANES
    gu = [interleaved(wg, wu, l, wgu.at[l], sem.at[l]) for l in range(2)]
    down = [pltpu.make_async_copy(wd.at[l], wdv.at[l], sem.at[2 + l]) for l in range(2)]
    first = pl.program_id(0) == 0

    @pl.when(first)
    def _():
        for l in range(2):
            for c in gu[l]:
                c.start()
            down[l].start()
        pltpu.make_async_copy(wgu.at[0], wgu.at[0], sem.at[0]).wait()

    x = x_ref[...]
    a0 = normed(x)
    a0_ref[...] = a0
    a0t_ref[...] = a0.T
    for j in range(blocks):
        both = dot(a0, wgu[0, :, 2 * j * LANES : 2 * (j + 1) * LANES])
        gate, up = both[:, :LANES], both[:, LANES:]
        mid = (gate * jax.nn.sigmoid(gate) * up).astype(BF16)
        mid0[:, j * LANES : (j + 1) * LANES] = mid
        mid0t_ref[j * LANES : (j + 1) * LANES, :] = mid.T

    @pl.when(first)
    def _():
        down[0].wait()

    h1 = x + dot(mid0[...], wdv[0]).astype(BF16)
    h1_ref[...] = h1
    a1 = normed(h1)
    a1t_ref[...] = a1.T

    @pl.when(first)
    def _():
        pltpu.make_async_copy(wgu.at[1], wgu.at[1], sem.at[1]).wait()
        down[1].wait()

    dy = dy_ref[...]
    for pair, width in pairs(blocks):
        dp2 = dot_t(dy, wdv[1, pair * LANES : (pair + width) * LANES, :]).astype(BF16).astype(F32)
        for j in range(pair, pair + width):
            at = slice(j * LANES, (j + 1) * LANES)
            both = dot(a1, wgu[1, :, 2 * j * LANES : 2 * (j + 1) * LANES])
            gate, up = both[:, :LANES], both[:, LANES:]
            silu, dg, du = backward_of_product(gate, up, dp2[:, (j - pair) * LANES : (j - pair + 1) * LANES])
            mid1t_ref[at, :] = (silu * up).astype(BF16).T
            dg_ref[:, at], du_ref[:, at] = dg, du


def forward(x, dy, wg, wu, wd, bt=256):
    t, d = x.shape
    ff = wg.shape[-1]
    rows = lambda n: pl.BlockSpec((bt, n), lambda i: (i, 0))
    cols = lambda n: pl.BlockSpec((n, bt), lambda i: (0, i))
    shape = lambda *s: jax.ShapeDtypeStruct(s, BF16)
    return pl.pallas_call(
        forward_kernel,
        grid=(t // bt,),
        in_specs=[rows(d), rows(d), ANY, ANY, ANY],
        out_specs=[rows(d), cols(d), rows(d), cols(d), cols(ff), cols(ff), rows(ff), rows(ff)],
        out_shape=[shape(t, d), shape(d, t), shape(t, d), shape(d, t), shape(ff, t), shape(ff, t), shape(t, ff), shape(t, ff)],
        scratch_shapes=[
            pltpu.VMEM((2, d, 2 * ff), BF16),
            pltpu.VMEM((2, ff, d), BF16),
            pltpu.VMEM((bt, ff), BF16),
            pltpu.SemaphoreType.DMA((4,)),
        ],
        compiler_params=pltpu.CompilerParams(dimension_semantics=("arbitrary",), vmem_limit_bytes=60 * 2**20),
        name="forward",
    )(x, dy, wg, wu, wd)


ORDER = ((True, 0, 1), (False, 0, 1), (False, 1, 1), (True, 1, 0), (False, 2, 0), (False, 3, 0))
S0, X1, X2, Y2, Y1, Y0 = 0, 1, 3, 5, 7, 9


def backward_kernel(
    a0, a0t, h1, a1t, mid0t, mid1t, dg1, du1, dy, wg, wu, wd,
    out_g, out_u, out_d,
    gg, gd, r0g, r0d, r1g, r1d, r2g, r2d,
    midt, dgu, at, av, dh, hv, wgu0, wgu1, wd0,
    load, store, send, recv, credit,
):
    t, d = dh.shape
    ff = wd0.shape[0]
    blocks = ff // LANES
    bt = 256
    index = lax.axis_index("dp")
    core, chip = index % 2, index // 2
    parity = chip % 2
    chips = lax.axis_size("dp") // 2
    up_chip, down_chip = (chip + 1) % chips, (chip + chips - 1) % chips
    first_pair = jnp.where(parity == 0, up_chip, down_chip)
    second_pair = jnp.where(parity == 0, down_chip, up_chip)
    other_core = chip * 2 + 1 - core
    near = (first_pair * 2 + core, second_pair * 2 + core)
    far = (near[1], near[0])
    middle = ((chip + 1) % chips) // 2
    keep = (middle, chip // 2)
    quarter = parity

    def height(m):
        return ff if ORDER[m][0] else d // 2

    def g_ref(m, half, start, size):
        is_down, i, _ = ORDER[m]
        if is_down:
            return gd.at[i, half, pl.ds(pl.multiple_of(start, 16), size), :]
        return gg.at[i, pl.ds(pl.multiple_of(half * (d // 2) + start, 16), size), :]

    def ref_of(m, down_ref, other_ref, *at):
        is_down, i, _ = ORDER[m]
        return (down_ref if is_down else other_ref).at[(i, *at)]

    def part(ref, start, size):
        return ref.at[pl.ds(pl.multiple_of(start, 16), size), :]

    def copy(m, kind, src, dst, device):
        return pltpu.make_async_remote_copy(
            src_ref=src, dst_ref=dst, send_sem=send.at[m, kind], recv_sem=recv.at[m, kind], device_id={"dp": device}, device_id_type=MESH
        )

    def sub_at(m, ab, which):
        sub = height(m) // 4
        return ab * 2 * sub + which * sub

    def s0(m):
        return copy(m, S0, g_ref(m, 1 - core, 0, height(m)), ref_of(m, r0d, r0g), other_core)

    def x1(m, ab):
        sub = height(m) // 4
        return copy(m, X1 + ab, part(ref_of(m, r0d, r0g), sub_at(m, ab, 1 - keep[ab]), sub), ref_of(m, r1d, r1g, ab), near[ab])

    def x2(m, ab):
        q = height(m) // 8
        return copy(m, X2 + ab, part(ref_of(m, r1d, r1g, ab), (1 - quarter) * q, q), ref_of(m, r2d, r2g, ab), far[ab])

    def y2(m, ab):
        q = height(m) // 8
        ref = g_ref(m, core, sub_at(m, ab, keep[ab]) + quarter * q, q)
        return copy(m, Y2 + ab, ref, ref, far[ab])

    def y1(m, ab):
        ref = g_ref(m, core, sub_at(m, ab, keep[ab]), height(m) // 4)
        return copy(m, Y1 + ab, ref, ref, near[ab])

    def y0(m):
        ref = g_ref(m, core, 0, height(m))
        return copy(m, Y0, ref, ref, other_core)

    def outs(m):
        is_down, i, layer = ORDER[m]
        if is_down:
            return [
                pltpu.make_async_copy(gd.at[i, h], out_d.at[layer, :, pl.ds(h * (d // 2), d // 2)], store.at[m, h]) for h in range(2)
            ]
        return [pltpu.make_async_copy(gg.at[i], (out_u if i % 2 else out_g).at[layer], store.at[m, 0])]

    def added(a, b):
        return (a[...].astype(F32) + b[...].astype(F32)).astype(BF16)

    def c0(m):
        s0(m).wait_recv()
        r0 = ref_of(m, r0d, r0g)
        r0[...] = added(r0, g_ref(m, core, 0, height(m)))
        for ab in range(2):
            x1(m, ab).start()
        s0(m).wait_send()
        pl.semaphore_signal(credit.at[m], inc=1, device_id={"dp": other_core}, device_id_type=MESH)

    def c1(m):
        sub = height(m) // 4
        for ab in range(2):
            x1(m, ab).wait_recv()
            r1 = ref_of(m, r1d, r1g, ab)
            r1[...] = added(r1, part(ref_of(m, r0d, r0g), sub_at(m, ab, keep[ab]), sub))
            x2(m, ab).start()

    def c2(m):
        q = height(m) // 8
        for ab in range(2):
            x2(m, ab).wait_recv()
            to = g_ref(m, core, sub_at(m, ab, keep[ab]) + quarter * q, q)
            to[...] = added(part(ref_of(m, r1d, r1g, ab), quarter * q, q), ref_of(m, r2d, r2g, ab))
            y2(m, ab).start()

    def c3(m):
        for ab in range(2):
            y2(m, ab).wait_recv()
            y1(m, ab).start()

    def c4(m):
        for ab in range(2):
            y1(m, ab).wait_recv()
        pl.semaphore_wait(credit.at[m], 1)
        y0(m).start()

    def c5(m):
        y0(m).wait_recv()
        for c in outs(m):
            c.start()

    def finish(m):
        for ab in range(2):
            for c in (x1, x2, y2, y1):
                c(m, ab).wait_send()
        y0(m).wait_send()
        for c in outs(m):
            c.wait()

    def run(step, table):
        for when, todo in table.items():

            @pl.when(step == when)
            def _():
                for what, m in todo:
                    what(m)

    local = {
        "mid1": pltpu.make_async_copy(mid1t, midt, load.at[0]),
        "dy": pltpu.make_async_copy(dy, dh, load.at[1]),
        "a1": pltpu.make_async_copy(a1t, at, load.at[2]),
        "dg": pltpu.make_async_copy(dg1, dgu.at[0], load.at[3]),
        "du": pltpu.make_async_copy(du1, dgu.at[1], load.at[4]),
        "h1": pltpu.make_async_copy(h1, hv, load.at[5]),
        "wg1": pltpu.make_async_copy(wg.at[1], wgu1.at[0], load.at[6]),
        "wu1": pltpu.make_async_copy(wu.at[1], wgu1.at[1], load.at[7]),
        "mid0": pltpu.make_async_copy(mid0t, midt, load.at[8]),
        "wd0": pltpu.make_async_copy(wd.at[0], wd0, load.at[9]),
        "a0": pltpu.make_async_copy(a0, av, load.at[10]),
        "a0t": pltpu.make_async_copy(a0t, at, load.at[11]),
    }
    for name in ("mid1", "dy", "a1", "dg", "du", "h1", "wg1", "wu1", "wd0", "a0"):
        local[name].start()
    for c in interleaved(wg, wu, 0, wgu0, load.at[12]):
        c.start()

    barrier = pltpu.get_barrier_semaphore()
    for other in (other_core, *near):
        pl.semaphore_signal(barrier, inc=1, device_id={"dp": other}, device_id_type=MESH)

    half = d // 2

    def down_grad(m, table):
        i = ORDER[m][1]

        def body(step, carry):
            which = jnp.where(step == 0, 1 - core, core)
            gd[i, which] = dot(midt[...], dh[:, pl.ds(pl.multiple_of(which * half, half), half)]).astype(BF16)

            @pl.when(step == 0)
            def _():
                s0(m).start()

            run(step, table)
            return carry

        lax.fori_loop(0, 2, body, 0)

    def other_grads(m, table):
        i = ORDER[m][1]

        def body(step, carry):
            which = jnp.where(step % 2 == 0, 1 - core, core)
            rows = pl.ds(pl.multiple_of(which * half, half), half)
            gg[i + step // 2, rows, :] = dot(at[rows, :], dgu[step // 2]).astype(BF16)
            for n in range(2):

                @pl.when(step == 2 * n)
                def _():
                    s0(m + n).start()

            run(step, table)
            return carry

        lax.fori_loop(0, 4, body, 0)

    local["mid1"].wait()
    local["dy"].wait()
    pl.semaphore_wait(barrier, 3)
    down_grad(0, {})
    local["mid0"].start()
    local["a1"].wait()
    local["dg"].wait()
    local["du"].wait()
    other_grads(1, {0: [(c0, 0)], 2: [(c0, 1)], 3: [(c1, 0)]})
    local["a0t"].start()
    local["h1"].wait()
    local["wg1"].wait()
    local["wu1"].wait()

    def states_grad(step, carry):
        rows = pl.ds(pl.multiple_of(step * bt, bt), bt)
        by_a = dot_t(dgu[0, rows, :], wgu1[0]).astype(BF16) + dot_t(dgu[1, rows, :], wgu1[1]).astype(BF16)
        by_a = by_a.astype(F32)
        wide = hv[rows, :].astype(F32)
        scale = lax.rsqrt(jnp.mean(wide * wide, -1, keepdims=True) + 1e-6)
        along = jnp.mean(by_a * wide, -1, keepdims=True) * (scale * scale * scale)
        dh[rows, :] = dh[rows, :] + (by_a * scale - wide * along).astype(BF16)
        run(step, {0: [(c0, 2)], 3: [(c1, 1)], 4: [(c2, 0)], 6: [(c1, 2)], 7: [(c3, 0)]})
        return carry

    lax.fori_loop(0, t // bt, states_grad, 0)

    local["mid0"].wait()
    down_grad(3, {0: [(c2, 1)], 1: [(c2, 2), (c0, 3)]})
    local["wd0"].wait()
    local["a0"].wait()
    pltpu.make_async_copy(wgu0, wgu0, load.at[12]).wait()

    def layer_back(step, carry):
        rows = pl.ds(pl.multiple_of(step * bt, bt), bt)
        a, by_h = av[rows, :], dh[rows, :]
        for pair, width in pairs(blocks):
            dp2 = dot_t(by_h, wd0[pair * LANES : (pair + width) * LANES, :]).astype(BF16).astype(F32)
            for j in range(pair, pair + width):
                to = slice(j * LANES, (j + 1) * LANES)
                both = dot(a, wgu0[:, 2 * j * LANES : 2 * (j + 1) * LANES])
                _, dg, du = backward_of_product(both[:, :LANES], both[:, LANES:], dp2[:, (j - pair) * LANES : (j - pair + 1) * LANES])
                dgu[0, rows, to], dgu[1, rows, to] = dg, du
        run(step, {0: [(c4, 0)], 1: [(c3, 1)], 3: [(c1, 3)], 4: [(c3, 2)], 5: [(c5, 0)], 6: [(c4, 1)], 7: [(c2, 3)]})
        return carry

    lax.fori_loop(0, t // bt, layer_back, 0)
    local["a0t"].wait()
    other_grads(4, {0: [(c4, 2)], 1: [(c0, 4), (c5, 1)], 3: [(c0, 5), (c3, 3)]})
    tail = [(c1, 4), (c5, 2), (c1, 5), (c4, 3), (c2, 4), (c5, 3), (c2, 5), (c3, 4), (c3, 5), (c4, 4), (c5, 4), (c4, 5), (c5, 5)]
    for what, m in tail:
        what(m)
    for m in range(6):
        finish(m)


def backward(a0, a0t, h1, a1t, mid0t, mid1t, dg1, du1, dy, wg, wu, wd):
    t, d = dy.shape
    layers, _, ff = wg.shape
    half = d // 2
    vmem = lambda *s: pltpu.VMEM(s, BF16)
    return pl.pallas_call(
        backward_kernel,
        in_specs=[ANY] * 12,
        out_specs=[ANY] * 3,
        out_shape=[jax.ShapeDtypeStruct(w.shape, BF16) for w in (wg, wu, wd)],
        scratch_shapes=[
            vmem(4, d, ff),
            vmem(2, 2, ff, half),
            vmem(4, half, ff),
            vmem(2, ff, half),
            vmem(4, 2, half // 4, ff),
            vmem(2, 2, ff // 4, half),
            vmem(4, 2, half // 8, ff),
            vmem(2, 2, ff // 8, half),
            vmem(ff, t),
            vmem(2, t, ff),
            vmem(d, t),
            vmem(t, d),
            vmem(t, d),
            vmem(t, d),
            vmem(d, 2 * ff),
            vmem(2, d, ff),
            vmem(ff, d),
            pltpu.SemaphoreType.DMA((13,)),
            pltpu.SemaphoreType.DMA((6, 2)),
            pltpu.SemaphoreType.DMA((6, 10)),
            pltpu.SemaphoreType.DMA((6, 10)),
            pltpu.SemaphoreType.REGULAR((6,)),
        ],
        compiler_params=pltpu.CompilerParams(collective_id=0, has_side_effects=True, vmem_limit_bytes=67043328),
        name="backward",
    )(a0, a0t, h1, a1t, mid0t, mid1t, dg1, du1, dy, wg, wu, wd)


def adamw_kernel(*refs):
    ins, outs = refs[:12], refs[12:]
    for n in range(3):
        w, m, v, g = (ins[n + 3 * k][...].astype(F32) for k in range(4))
        m = 0.9 * m + 0.1 * g
        v = 0.95 * v + 0.05 * g * g
        step = m * lax.rsqrt(v + 1e-8) + 0.1 * w
        outs[n][...] = (w - 0.02 * step).astype(BF16)
        outs[n + 3][...] = m
        outs[n + 6][...] = v


def adamw(weights, m, v, g, parts=8):
    specs = [pl.BlockSpec((1, w.shape[1] // parts, w.shape[2]), lambda l, i: (l, i, 0)) for w in weights]
    shapes = [jax.ShapeDtypeStruct(w.shape, kind) for kind in (BF16, F32, F32) for w in weights]
    return pl.pallas_call(
        adamw_kernel,
        grid=(weights[0].shape[0], parts),
        in_specs=specs * 4,
        out_specs=specs * 3,
        out_shape=shapes,
        compiler_params=pltpu.CompilerParams(dimension_semantics=("arbitrary",) * 2, vmem_limit_bytes=60 * 2**20),
        name="adamw",
    )(*weights, *m, *v, *g)


def solution(mesh):
    def step(x, dy, *arrays):
        weights, m, v = (arrays[i : i + 3] for i in (0, 3, 6))
        made = forward(x[0], dy[0], *weights)
        return tuple(adamw(weights, m, v, backward(*made, dy[0], *weights)))

    return jax.shard_map(
        step,
        mesh=mesh,
        in_specs=(P(("rep", "dp"), None, None),) * 2 + (P(None, None, None),) * 9,
        out_specs=(P("rep", None, None),) * 9,
        check_vma=False,
    )
```

```python
import jax
import jax.numpy as jnp
from jax import lax
from jax.experimental import pallas as pl
from jax.experimental.pallas import tpu as pltpu
from jax.sharding import PartitionSpec as P

HBM = pl.BlockSpec(memory_space=pltpu.HBM)
VMEM = pl.BlockSpec(memory_space=pltpu.VMEM)
LANES = 128
BF16, F32 = jnp.bfloat16, jnp.float32
MESH = pl.DeviceIdType.MESH


def dot(a, b, dims=((1,), (0,))):
    return lax.dot_general(a, b, (dims, ((), ())), preferred_element_type=F32)


def dot_t(a, b):
    return dot(a, b, ((1,), (1,)))


def normed(h):
    wide = h.astype(F32)
    scale = lax.rsqrt(jnp.mean(wide * wide, -1, keepdims=True) + 1e-6)
    return (wide * scale).astype(BF16)


def interleaved(wg, wu, layer, to, sem):
    out = []
    for j in range(wg.shape[2] // LANES):
        for n, w in enumerate((wg, wu)):
            out.append(pltpu.make_async_copy(w.at[layer, :, pl.ds(j * LANES, LANES)], to.at[:, pl.ds((2 * j + n) * LANES, LANES)], sem))
    return out


def pairs(blocks):
    return [(at, min(2, blocks - at)) for at in range(0, blocks, 2)]


def backward_of_product(gate, up, dp):
    s = jax.nn.sigmoid(gate)
    silu = gate * s
    return silu, (dp * up * (s + silu * (1 - s))).astype(BF16), (dp * silu).astype(BF16)


def forward_kernel(x_ref, dy_ref, wg, wu, wd, a0_ref, a0t_ref, h1_ref, a1t_ref, mid0t_ref, mid1t_ref, dg_ref, du_ref, wgu, wdv, mid0, sem):
    blocks = wg.shape[2] // LANES
    gu = [interleaved(wg, wu, l, wgu.at[l], sem.at[l]) for l in range(2)]
    down = [pltpu.make_async_copy(wd.at[l], wdv.at[l], sem.at[2 + l]) for l in range(2)]
    first = pl.program_id(0) == 0

    @pl.when(first)
    def _():
        for l in range(2):
            for c in gu[l]:
                c.start()
            down[l].start()
        pltpu.make_async_copy(wgu.at[0], wgu.at[0], sem.at[0]).wait()

    x = x_ref[...]
    a0 = normed(x)
    a0_ref[...] = a0
    a0t_ref[...] = a0.T
    for j in range(blocks):
        both = dot(a0, wgu[0, :, 2 * j * LANES : 2 * (j + 1) * LANES])
        gate, up = both[:, :LANES], both[:, LANES:]
        mid = (gate * jax.nn.sigmoid(gate) * up).astype(BF16)
        mid0[:, j * LANES : (j + 1) * LANES] = mid
        mid0t_ref[j * LANES : (j + 1) * LANES, :] = mid.T

    @pl.when(first)
    def _():
        down[0].wait()

    h1 = x + dot(mid0[...], wdv[0]).astype(BF16)
    h1_ref[...] = h1
    a1 = normed(h1)
    a1t_ref[...] = a1.T

    @pl.when(first)
    def _():
        pltpu.make_async_copy(wgu.at[1], wgu.at[1], sem.at[1]).wait()
        down[1].wait()

    dy = dy_ref[...]
    for pair, width in pairs(blocks):
        dp2 = dot_t(dy, wdv[1, pair * LANES : (pair + width) * LANES, :]).astype(BF16).astype(F32)
        for j in range(pair, pair + width):
            at = slice(j * LANES, (j + 1) * LANES)
            both = dot(a1, wgu[1, :, 2 * j * LANES : 2 * (j + 1) * LANES])
            gate, up = both[:, :LANES], both[:, LANES:]
            silu, dg, du = backward_of_product(gate, up, dp2[:, (j - pair) * LANES : (j - pair + 1) * LANES])
            mid1t_ref[at, :] = (silu * up).astype(BF16).T
            dg_ref[:, at], du_ref[:, at] = dg, du


def forward(x, dy, wg, wu, wd, bt=256):
    t, d = x.shape
    ff = wg.shape[-1]
    rows = lambda n: pl.BlockSpec((bt, n), lambda i: (i, 0))
    cols = lambda n: pl.BlockSpec((n, bt), lambda i: (0, i))
    shape = lambda *s: jax.ShapeDtypeStruct(s, BF16)
    return pl.pallas_call(
        forward_kernel,
        grid=(t // bt,),
        in_specs=[rows(d), rows(d), HBM, HBM, HBM],
        out_specs=[rows(d), cols(d), rows(d), cols(d), cols(ff), cols(ff), rows(ff), rows(ff)],
        out_shape=[shape(t, d), shape(d, t), shape(t, d), shape(d, t), shape(ff, t), shape(ff, t), shape(t, ff), shape(t, ff)],
        scratch_shapes=[
            pltpu.VMEM((2, d, 2 * ff), BF16),
            pltpu.VMEM((2, ff, d), BF16),
            pltpu.VMEM((bt, ff), BF16),
            pltpu.SemaphoreType.DMA((4,)),
        ],
        compiler_params=pltpu.CompilerParams(dimension_semantics=("arbitrary",), vmem_limit_bytes=60 * 2**20),
        name="forward",
    )(x, dy, wg, wu, wd)


ORDER = ((True, 0, 1), (False, 0, 1), (False, 1, 1), (True, 0, 0), (False, 0, 0), (False, 1, 0))
S0, X1, X2, Y2, Y1, Y0, YR = 0, 2, 4, 6, 8, 10, 12


class Places:
    def __init__(self, tokens_d, ff):
        self.d, self.ff = tokens_d, ff
        index = lax.axis_index("dp")
        self.core, chip = index % 2, index // 2
        chips = lax.axis_size("dp") // 2
        self.quarter = chip % 2
        after, before = (chip + 1) % chips, (chip + chips - 1) % chips
        first = jnp.where(self.quarter == 0, after, before)
        second = jnp.where(self.quarter == 0, before, after)
        self.other_core = chip * 2 + 1 - self.core
        self.near = (first * 2 + self.core, second * 2 + self.core)
        self.far = (self.near[1], self.near[0])
        self.keep = (((chip + 1) % chips) // 2, chip // 2)

    def height(self, m):
        return self.ff if ORDER[m][0] else self.d // 2

    def sub_at(self, m, ab, which):
        sub = self.height(m) // 4
        return (2 * ab + which) * sub

    def share(self, m, down, other, half, start, size):
        if ORDER[m][0]:
            return down.at[half, pl.ds(pl.multiple_of(start, 16), size), :]
        return other.at[ORDER[m][1], pl.ds(pl.multiple_of(half * (self.d // 2) + start, 16), size), :]

    def greet(self):
        barrier = pltpu.get_barrier_semaphore()
        for other in (self.other_core, *self.near):
            pl.semaphore_signal(barrier, inc=1, device_id={"dp": other}, device_id_type=MESH)


def part(ref, start, size):
    return ref.at[pl.ds(pl.multiple_of(start, 16), size), :]


def added(a, b):
    return (a[...].astype(F32) + b[...].astype(F32)).astype(BF16)


def backward_kernel(
    a0, a0t, h1, a1t, mid0t, mid1t, dg1, du1, dy, wg, wu, wd,
    done_g, done_d, own_g, own_d,
    gg1, gd1, gg0, gd0, r0g, r0d, r1g, r1d, r2g, r2d,
    midt, dgu, at, av, dh, hv, wgu0, wgu1, wd0,
    load, store, quarters, send, recv, credit,
):
    t, d = dh.shape
    ff = wd0.shape[0]
    blocks = ff // LANES
    bt = 256
    half = d // 2
    p = Places(d, ff)

    def g_ref(m, half, start, size):
        return p.share(m, *((gd1, gg1) if ORDER[m][2] else (gd0, gg0)), half, start, size)

    def ref_of(m, down_ref, other_ref, *at):
        is_down, i, layer = ORDER[m]
        i = layer if is_down else 2 * layer + i
        return (down_ref if is_down else other_ref).at[(i, *at)]

    def copy(m, kind, src, dst, device):
        return pltpu.make_async_remote_copy(
            src_ref=src, dst_ref=dst, send_sem=send.at[m, kind], recv_sem=recv.at[m, kind], device_id={"dp": device}, device_id_type=MESH
        )

    def s0(m, ab):
        size = p.height(m) // 2
        return copy(m, S0 + ab, g_ref(m, 1 - p.core, ab * size, size), part(ref_of(m, r0d, r0g), ab * size, size), p.other_core)

    def x1(m, ab):
        src = part(ref_of(m, r0d, r0g), p.sub_at(m, ab, 1 - p.keep[ab]), p.height(m) // 4)
        return copy(m, X1 + ab, src, ref_of(m, r1d, r1g, ab), p.near[ab])

    def x2(m, ab):
        q = p.height(m) // 8
        return copy(m, X2 + ab, part(ref_of(m, r1d, r1g, ab), (1 - p.quarter) * q, q), ref_of(m, r2d, r2g, ab), p.far[ab])

    def y2(m, ab):
        q = p.height(m) // 8
        ref = g_ref(m, p.core, p.sub_at(m, ab, p.keep[ab]) + p.quarter * q, q)
        return copy(m, Y2 + ab, ref, ref, p.far[ab])

    def y1(m, ab):
        ref = g_ref(m, p.core, p.sub_at(m, ab, p.keep[ab]), p.height(m) // 4)
        return copy(m, Y1 + ab, ref, ref, p.near[ab])

    def y0(m):
        ref = g_ref(m, p.core, 0, p.height(m))
        return copy(m, Y0, ref, ref, p.other_core)

    def out(m):
        is_down, i, _ = ORDER[m]
        if is_down:
            return pltpu.make_async_copy(gd1, done_d, store.at[m])
        return pltpu.make_async_copy(gg1.at[i], done_g.at[i], store.at[m])

    def out_quarter(m, ab):
        to = own_d.at[ab] if ORDER[m][0] else own_g.at[ORDER[m][1], ab]
        return pltpu.make_async_copy(ref_of(m, r2d, r2g, ab), to, quarters.at[m - 3, ab])

    def c0(m, parts=(0, 1)):
        size = p.height(m) // 2
        for ab in parts:
            s0(m, ab).wait_recv()
            r0 = part(ref_of(m, r0d, r0g), ab * size, size)
            r0[...] = added(r0, g_ref(m, p.core, ab * size, size))
            x1(m, ab).start()
        for ab in parts:
            s0(m, ab).wait_send()
        if ORDER[m][2] and 1 in parts:
            pl.semaphore_signal(credit.at[m], inc=1, device_id={"dp": p.other_core}, device_id_type=MESH)

    def c0a(m):
        c0(m, (0,))

    def c0b(m):
        c0(m, (1,))

    def c1(m):
        for ab in range(2):
            x1(m, ab).wait_recv()
            r1 = ref_of(m, r1d, r1g, ab)
            r1[...] = added(r1, part(ref_of(m, r0d, r0g), p.sub_at(m, ab, p.keep[ab]), p.height(m) // 4))
            x2(m, ab).start()

    def c2(m):
        q = p.height(m) // 8
        for ab in range(2):
            x2(m, ab).wait_recv()
            if ORDER[m][2]:
                to = g_ref(m, p.core, p.sub_at(m, ab, p.keep[ab]) + p.quarter * q, q)
            else:
                to = ref_of(m, r2d, r2g, ab)
            to[...] = added(part(ref_of(m, r1d, r1g, ab), p.quarter * q, q), ref_of(m, r2d, r2g, ab))
            if ORDER[m][2]:
                y2(m, ab).start()
            else:
                out_quarter(m, ab).start()

    def c3(m):
        for ab in range(2):
            y2(m, ab).wait_recv()
            y1(m, ab).start()

    def c4(m):
        for ab in range(2):
            y1(m, ab).wait_recv()
        pl.semaphore_wait(credit.at[m], 1)
        y0(m).start()

    def c5(m):
        y0(m).wait_recv()
        out(m).start()

    def finish(m):
        for ab in range(2):
            for c in (x1, x2, y2, y1) if ORDER[m][2] else (x1, x2):
                c(m, ab).wait_send()
        if ORDER[m][2]:
            y0(m).wait_send()
            out(m).wait()
        else:
            for ab in range(2):
                out_quarter(m, ab).wait()

    def run(step, table):
        for when, todo in table.items():

            @pl.when(step == when)
            def _():
                for what, m in todo:
                    what(m)

    local = {
        "mid1": pltpu.make_async_copy(mid1t, midt, load.at[0]),
        "dy": pltpu.make_async_copy(dy, dh, load.at[1]),
        "a1": pltpu.make_async_copy(a1t, at, load.at[2]),
        "dg": pltpu.make_async_copy(dg1, dgu.at[0], load.at[3]),
        "du": pltpu.make_async_copy(du1, dgu.at[1], load.at[4]),
        "h1": pltpu.make_async_copy(h1, hv, load.at[5]),
        "wg1": pltpu.make_async_copy(wg.at[1], wgu1.at[0], load.at[6]),
        "wu1": pltpu.make_async_copy(wu.at[1], wgu1.at[1], load.at[7]),
        "mid0": pltpu.make_async_copy(mid0t, midt, load.at[8]),
        "wd0": pltpu.make_async_copy(wd.at[0], wd0, load.at[9]),
        "a0": pltpu.make_async_copy(a0, av, load.at[10]),
        "a0t": pltpu.make_async_copy(a0t, at, load.at[11]),
    }
    p.greet()
    for name in ("dy", "mid1", "a1", "dg", "du", "h1", "wg1", "wu1", "wd0", "a0"):
        local[name].start()
    for c in interleaved(wg, wu, 0, wgu0, load.at[12]):
        c.start()

    def down_grad(m, gd, table):
        def body(step, carry):
            which = jnp.where(step < 2, 1 - p.core, p.core)
            rows = pl.ds(pl.multiple_of((step % 2) * (ff // 2), 16), ff // 2)
            gd[which, rows, :] = dot(midt[rows, :], dh[:, pl.ds(pl.multiple_of(which * half, half), half)]).astype(BF16)
            for ab in range(2):

                @pl.when(step == ab)
                def _():
                    s0(m, ab).start()

            run(step, table)
            return carry

        lax.fori_loop(0, 4, body, 0)

    def other_grads(m, gg, table):
        def body(step, carry):
            which = jnp.where(step % 2 == 0, 1 - p.core, p.core)
            rows = pl.ds(pl.multiple_of(which * half, half), half)
            gg[step // 2, rows, :] = dot(at[rows, :], dgu[step // 2]).astype(BF16)
            for n in range(2):

                @pl.when(step == 2 * n)
                def _():
                    for ab in range(2):
                        s0(m + n, ab).start()

            run(step, table)
            return carry

        lax.fori_loop(0, 4, body, 0)

    local["dy"].wait()
    local["mid1"].wait()
    pl.semaphore_wait(pltpu.get_barrier_semaphore(), 3)
    down_grad(0, gd1, {2: [(c0a, 0)], 3: [(c0b, 0)]})
    local["mid0"].start()
    local["a1"].wait()
    local["dg"].wait()
    local["du"].wait()
    other_grads(1, gg1, {1: [(c1, 0), (c0, 1)], 3: [(c2, 0)]})
    local["a0t"].start()
    local["h1"].wait()
    local["wg1"].wait()
    local["wu1"].wait()

    def states_grad(step, carry):
        rows = pl.ds(pl.multiple_of(step * bt, bt), bt)
        by_a = dot_t(dgu[0, rows, :], wgu1[0]).astype(BF16) + dot_t(dgu[1, rows, :], wgu1[1]).astype(BF16)
        by_a = by_a.astype(F32)
        wide = hv[rows, :].astype(F32)
        scale = lax.rsqrt(jnp.mean(wide * wide, -1, keepdims=True) + 1e-6)
        along = jnp.mean(by_a * wide, -1, keepdims=True) * (scale * scale * scale)
        dh[rows, :] = dh[rows, :] + (by_a * scale - wide * along).astype(BF16)
        run(step, {0: [(c0, 2)], 3: [(c1, 1)], 6: [(c1, 2)]})
        return carry

    lax.fori_loop(0, t // bt, states_grad, 0)

    local["mid0"].wait()
    down_grad(3, gd0, {1: [(c3, 0)], 2: [(c2, 1), (c0a, 3)], 3: [(c0b, 3)]})
    local["wd0"].wait()
    local["a0"].wait()
    pltpu.make_async_copy(wgu0, wgu0, load.at[12]).wait()

    def layer_back(step, carry):
        rows = pl.ds(pl.multiple_of(step * bt, bt), bt)
        a, by_h = av[rows, :], dh[rows, :]
        for pair, width in pairs(blocks):
            dp2 = dot_t(by_h, wd0[pair * LANES : (pair + width) * LANES, :]).astype(BF16).astype(F32)
            for j in range(pair, pair + width):
                to = slice(j * LANES, (j + 1) * LANES)
                both = dot(a, wgu0[:, 2 * j * LANES : 2 * (j + 1) * LANES])
                _, dg, du = backward_of_product(both[:, :LANES], both[:, LANES:], dp2[:, (j - pair) * LANES : (j - pair + 1) * LANES])
                dgu[0, rows, to], dgu[1, rows, to] = dg, du
        run(step, {0: [(c2, 2)], 2: [(c4, 0)], 4: [(c5, 0), (c3, 1)], 6: [(c1, 3)], 7: [(c3, 2)]})
        return carry

    lax.fori_loop(0, t // bt, layer_back, 0)
    local["a0t"].wait()
    other_grads(4, gg0, {1: [(c4, 1), (c0, 4)], 2: [(c2, 3), (c5, 1)], 3: [(c0, 5)]})
    for what, m in [(c4, 2), (c1, 4), (c5, 2), (c1, 5), (c2, 4), (c2, 5)]:
        what(m)
    for m in range(6):
        finish(m)


def backward(a0, a0t, h1, a1t, mid0t, mid1t, dg1, du1, dy, wg, wu, wd):
    t, d = dy.shape
    ff = wg.shape[2]
    half = d // 2
    vmem = lambda *s: pltpu.VMEM(s, BF16)
    return pl.pallas_call(
        backward_kernel,
        in_specs=[HBM] * 12,
        out_specs=[HBM] * 4,
        out_shape=[
            jax.ShapeDtypeStruct(s, BF16) for s in ((2, d, ff), (2, ff, half), (2, 2, half // 8, ff), (2, ff // 8, half))
        ],
        scratch_shapes=[
            vmem(2, d, ff),
            vmem(2, ff, half),
            vmem(2, d, ff),
            vmem(2, ff, half),
            vmem(4, half, ff),
            vmem(2, ff, half),
            vmem(4, 2, half // 4, ff),
            vmem(2, 2, ff // 4, half),
            vmem(4, 2, half // 8, ff),
            vmem(2, 2, ff // 8, half),
            vmem(ff, t),
            vmem(2, t, ff),
            vmem(d, t),
            vmem(t, d),
            vmem(t, d),
            vmem(t, d),
            vmem(d, 2 * ff),
            vmem(2, d, ff),
            vmem(ff, d),
            pltpu.SemaphoreType.DMA((13,)),
            pltpu.SemaphoreType.DMA((3,)),
            pltpu.SemaphoreType.DMA((3, 2)),
            pltpu.SemaphoreType.DMA((6, 11)),
            pltpu.SemaphoreType.DMA((6, 11)),
            pltpu.SemaphoreType.REGULAR((3,)),
        ],
        compiler_params=pltpu.CompilerParams(collective_id=0, has_side_effects=True, vmem_limit_bytes=67043328),
        name="backward",
    )(a0, a0t, h1, a1t, mid0t, mid1t, dg1, du1, dy, wg, wu, wd)


def update_kernel(
    quarter_g, quarter_d, done_g, done_d, wg, wu, wd, mg, mu, md, vg, vu, vd,
    fg, fd, mg_out, mu_out, md_out, vg_out, vu_out, vd_out,
    own_g, own_d, load, quarters, send, recv,
):
    d, ff = wg.shape[1:]
    half = d // 2
    p = Places(d, ff)

    def f_ref(m, half, start, size):
        layer = ORDER[m][2]
        return p.share(m, fd.at[layer], fg.at[layer], half, start, size)

    def copy(m, kind, src, dst, device):
        at = (m - 3, kind - Y2)
        return pltpu.make_async_remote_copy(
            src_ref=src, dst_ref=dst, send_sem=send.at[at], recv_sem=recv.at[at], device_id={"dp": device}, device_id_type=MESH
        )

    def own_quarter(m, ab):
        q = p.height(m) // 8
        return p.core, p.sub_at(m, ab, p.keep[ab]) + p.quarter * q, q

    def summed(m, ab):
        return quarter_d.at[ab] if ORDER[m][0] else quarter_g.at[ORDER[m][1], ab]

    def y2(m, ab):
        ref = f_ref(m, *own_quarter(m, ab))
        return copy(m, Y2 + ab, ref, ref, p.far[ab])

    def mine(m, ab):
        return pltpu.make_async_copy(summed(m, ab), f_ref(m, *own_quarter(m, ab)), quarters.at[m - 3, ab])

    def y1(m, ab):
        ref = f_ref(m, p.core, p.sub_at(m, ab, p.keep[ab]), p.height(m) // 4)
        return copy(m, Y1 + ab, ref, ref, p.near[ab])

    def y0(m, ab):
        ref = f_ref(m, p.core, p.sub_at(m, ab, p.keep[ab]), p.height(m) // 4)
        return copy(m, Y0 + ab, ref, ref, p.other_core)

    def yr(m, ab):
        ref = f_ref(m, p.core, p.sub_at(m, ab, 1 - p.keep[ab]), p.height(m) // 4)
        return copy(m, YR + ab, ref, ref, p.other_core)

    def loads(m):
        is_down, i, layer = ORDER[m]
        w, mom, var = ((wd, md, vd), (wg, mg, vg), (wu, mu, vu))[0 if is_down else 1 + i]
        mom_out, var_out = ((md_out, vd_out), (mg_out, vg_out), (mu_out, vu_out))[0 if is_down else 1 + i]
        rest = [
            pltpu.make_async_copy(mom.at[layer], mom_out.at[layer], load.at[m, 1]),
            pltpu.make_async_copy(var.at[layer], var_out.at[layer], load.at[m, 2]),
        ]
        if layer:
            if is_down:
                rest.append(pltpu.make_async_copy(done_d, fd.at[layer], load.at[m, 3]))
            else:
                rest.append(pltpu.make_async_copy(done_g.at[i], fg.at[layer, i], load.at[m, 3]))
        to = own_d if is_down else own_g.at[i]
        return pltpu.make_async_copy(w.at[layer], to, load.at[m, 0]), rest

    def adamw(m, half_of, ab, which):
        is_down, i, layer = ORDER[m]
        mom, var = ((md_out, vd_out), (mg_out, vg_out), (mu_out, vu_out))[0 if is_down else 1 + i]
        size = p.height(m) // 4
        start = p.sub_at(m, ab, which)
        if is_down:
            at = (pl.ds(pl.multiple_of(start, 16), size), pl.ds(pl.multiple_of(half_of * half, half), half))
            w = own_d[at]
        else:
            at = (pl.ds(pl.multiple_of(half_of * half + start, 16), size), slice(None))
            w = own_g[(i, *at)]
        w = w.astype(F32)
        f = f_ref(m, half_of, start, size)
        g = f[...].astype(F32)
        new_m = 0.9 * mom[(layer, *at)] + 0.1 * g
        new_v = 0.95 * var[(layer, *at)] + 0.05 * g * g
        f[...] = (w - 0.02 * (new_m * lax.rsqrt(new_v + 1e-8) + 0.1 * w)).astype(BF16)
        mom[(layer, *at)] = new_m
        var[(layer, *at)] = new_v

    def c3(m):
        q = p.height(m) // 8
        for ab in range(2):
            y2(m, ab).wait_recv()
            y1(m, ab).start()
        for ab in range(2):
            y0(m, ab).start()

    def c4(m):
        for ab in range(2):
            y1(m, ab).wait_recv()
            yr(m, ab).start()

    def whole(m):
        own, rest = loads(m)
        own.wait()
        for c in rest:
            c.wait()

        def body(n, carry):
            adamw(m, n // 4, (n // 2) % 2, n % 2)
            return carry

        lax.fori_loop(0, 8, body, 0)
        loads(m + 3)[0].start()

    def others_kept(m):
        own, rest = loads(m)
        own.wait()
        for c in rest:
            c.wait()
        for ab in range(2):
            y0(m, ab).wait_recv()
            adamw(m, 1 - p.core, ab, p.keep[ab])

    def the_rest(m):
        for ab in range(2):
            y2(m, ab).wait_send()
            y0(m, ab).wait_send()
            y1(m, ab).wait_send()
            adamw(m, p.core, ab, p.keep[ab])
        for ab in range(2):
            yr(m, ab).wait_send()
            adamw(m, p.core, ab, 1 - p.keep[ab])
        for ab in range(2):
            yr(m, ab).wait_recv()
            adamw(m, 1 - p.core, ab, 1 - p.keep[ab])

    p.greet()
    for m in (3, 4, 5):
        for ab in range(2):
            mine(m, ab).start()
    for m in range(6):
        own, rest = loads(m)
        if m < 3:
            own.start()
        for c in rest:
            c.start()
    pl.semaphore_wait(pltpu.get_barrier_semaphore(), 3)
    for m in (3, 4, 5):
        for ab in range(2):
            mine(m, ab).wait()
            y2(m, ab).start()
    whole(0)
    c3(3)
    whole(1)
    c3(4)
    whole(2)
    c3(5)
    others_kept(3)
    c4(3)
    the_rest(3)
    others_kept(4)
    c4(4)
    the_rest(4)
    others_kept(5)
    c4(5)
    the_rest(5)


def update(weights, m, v, done_g, done_d, own_g, own_d):
    _, d, ff = weights[0].shape
    half = d // 2
    return pl.pallas_call(
        update_kernel,
        in_specs=[HBM] * 13,
        out_specs=[VMEM] * 8,
        out_shape=[pltpu.VMEM((2, 2, d, ff), BF16), pltpu.VMEM((2, 2, ff, half), BF16)] + [pltpu.VMEM(one.shape, F32) for one in (*m, *v)],
        scratch_shapes=[
            pltpu.VMEM((2, d, ff), BF16),
            pltpu.VMEM((ff, d), BF16),
            pltpu.SemaphoreType.DMA((6, 4)),
            pltpu.SemaphoreType.DMA((3, 2)),
            pltpu.SemaphoreType.DMA((3, 8)),
            pltpu.SemaphoreType.DMA((3, 8)),
        ],
        compiler_params=pltpu.CompilerParams(collective_id=1, has_side_effects=True, vmem_limit_bytes=12 * 2**20),
        name="update",
    )(own_g, own_d, done_g, done_d, *weights, *m, *v)


def written_kernel(fg, fd, mg, mu, md, vg, vu, vd, wg_out, wu_out, wd_out, mg_out, mu_out, md_out, vg_out, vu_out, vd_out, sem):
    layers, _, d, ff = fg.shape
    half = d // 2
    copies = [(one, to) for one, to in zip((mg, mu, md, vg, vu, vd), (mg_out, mu_out, md_out, vg_out, vu_out, vd_out), strict=True)]
    for l in range(layers):
        copies += [(fg.at[l, 0], wg_out.at[l]), (fg.at[l, 1], wu_out.at[l])]
        copies += [(fd.at[l, h], wd_out.at[l, :, pl.ds(h * half, half)]) for h in range(2)]
    copies = [pltpu.make_async_copy(a, b, sem.at[n]) for n, (a, b) in enumerate(copies)]
    for c in copies:
        c.start()
    for c in copies:
        c.wait()


def written(weights, values):
    return pl.pallas_call(
        written_kernel,
        in_specs=[VMEM] * 8,
        out_specs=[HBM] * 9,
        out_shape=[jax.ShapeDtypeStruct(w.shape, kind) for kind in (BF16, F32, F32) for w in weights],
        scratch_shapes=[pltpu.SemaphoreType.DMA((14,))],
        compiler_params=pltpu.CompilerParams(vmem_limit_bytes=12 * 2**20),
        name="written",
    )(*(pltpu.with_memory_space_constraint(one, pltpu.VMEM) for one in values))


def solution(mesh):
    def step(x, dy, *arrays):
        weights, m, v = (arrays[i : i + 3] for i in (0, 3, 6))
        made = forward(x[0], dy[0], *weights)
        summed = backward(*made, dy[0], *weights)
        return tuple(written(weights, update(weights, m, v, *summed)))

    return jax.shard_map(
        step,
        mesh=mesh,
        in_specs=(P(("rep", "dp"), None, None),) * 2 + (P(None, None, None),) * 9,
        out_specs=(P("rep", None, None),) * 9,
        check_vma=False,
    )
```

```python
import jax
import jax.numpy as jnp
from jax import lax
from jax.experimental import pallas as pl
from jax.experimental.pallas import tpu as pltpu
from jax.sharding import PartitionSpec as P

HBM = pl.BlockSpec(memory_space=pltpu.HBM)
VMEM = pl.BlockSpec(memory_space=pltpu.VMEM)
LANES = 128
BF16, F32 = jnp.bfloat16, jnp.float32
MESH = pl.DeviceIdType.MESH


def dot(a, b, dims=((1,), (0,))):
    return lax.dot_general(a, b, (dims, ((), ())), preferred_element_type=F32)


def dot_t(a, b):
    return dot(a, b, ((1,), (1,)))


def normed(h):
    wide = h.astype(F32)
    scale = lax.rsqrt(jnp.mean(wide * wide, -1, keepdims=True) + 1e-6)
    return (wide * scale).astype(BF16)


def interleaved(wg, wu, layer, to, sem):
    out = []
    for j in range(wg.shape[2] // LANES):
        for n, w in enumerate((wg, wu)):
            out.append(pltpu.make_async_copy(w.at[layer, :, pl.ds(j * LANES, LANES)], to.at[:, pl.ds((2 * j + n) * LANES, LANES)], sem))
    return out


def pairs(blocks):
    return [(at, min(2, blocks - at)) for at in range(0, blocks, 2)]


def backward_of_product(gate, up, dp):
    s = jax.nn.sigmoid(gate)
    silu = gate * s
    return silu, (dp * up * (s + silu * (1 - s))).astype(BF16), (dp * silu).astype(BF16)


ORDER = ((True, 0, 1), (False, 0, 1), (False, 1, 1), (True, 0, 0), (False, 0, 0), (False, 1, 0))
S0, X1, X2, Y2, Y1, Y0, YR = 0, 2, 4, 6, 8, 10, 12


class Places:
    def __init__(self, tokens_d, ff):
        self.d, self.ff = tokens_d, ff
        index = lax.axis_index("dp")
        self.core, chip = index % 2, index // 2
        chips = lax.axis_size("dp") // 2
        self.quarter = chip % 2
        after, before = (chip + 1) % chips, (chip + chips - 1) % chips
        first = jnp.where(self.quarter == 0, after, before)
        second = jnp.where(self.quarter == 0, before, after)
        self.other_core = chip * 2 + 1 - self.core
        self.near = (first * 2 + self.core, second * 2 + self.core)
        self.far = (self.near[1], self.near[0])
        self.keep = (((chip + 1) % chips) // 2, chip // 2)

    def height(self, m):
        return self.ff if ORDER[m][0] else self.d // 2

    def sub_at(self, m, ab, which):
        sub = self.height(m) // 4
        return (2 * ab + which) * sub

    def share(self, m, down, other, half, start, size):
        if ORDER[m][0]:
            return down.at[half, pl.ds(pl.multiple_of(start, 16), size), :]
        return other.at[ORDER[m][1], pl.ds(pl.multiple_of(half * (self.d // 2) + start, 16), size), :]

    def greet(self):
        barrier = pltpu.get_barrier_semaphore()
        for other in (self.other_core, *self.near):
            pl.semaphore_signal(barrier, inc=1, device_id={"dp": other}, device_id_type=MESH)


def part(ref, start, size):
    return ref.at[pl.ds(pl.multiple_of(start, 16), size), :]


def added(a, b):
    return (a[...].astype(F32) + b[...].astype(F32)).astype(BF16)


def gradients_kernel(
    x, dy, wg, wu, wd,
    done_g, done_d, own_g, own_d, mid0t,
    gg1, gd1, gg0, gd0, r0g, r0d, r1g, r1d, r2g, r2d,
    midt, dgu, at, av, dh, hv, wgu0, wgu1, wdv, mid0, midt_out,
    load, mid_store, store, quarters, send, recv, credit,
):
    t, d = dh.shape
    ff = wdv.shape[1]
    blocks = ff // LANES
    bt, fb = 256, mid0.shape[0]
    half = d // 2
    p = Places(d, ff)

    def g_ref(m, half, start, size):
        return p.share(m, *((gd1, gg1) if ORDER[m][2] else (gd0, gg0)), half, start, size)

    def ref_of(m, down_ref, other_ref, *at):
        is_down, i, layer = ORDER[m]
        i = layer if is_down else 2 * layer + i
        return (down_ref if is_down else other_ref).at[(i, *at)]

    def copy(m, kind, src, dst, device):
        return pltpu.make_async_remote_copy(
            src_ref=src, dst_ref=dst, send_sem=send.at[m, kind], recv_sem=recv.at[m, kind], device_id={"dp": device}, device_id_type=MESH
        )

    def s0(m, ab):
        size = p.height(m) // 2
        return copy(m, S0 + ab, g_ref(m, 1 - p.core, ab * size, size), part(ref_of(m, r0d, r0g), ab * size, size), p.other_core)

    def x1(m, ab):
        src = part(ref_of(m, r0d, r0g), p.sub_at(m, ab, 1 - p.keep[ab]), p.height(m) // 4)
        return copy(m, X1 + ab, src, ref_of(m, r1d, r1g, ab), p.near[ab])

    def x2(m, ab):
        q = p.height(m) // 8
        return copy(m, X2 + ab, part(ref_of(m, r1d, r1g, ab), (1 - p.quarter) * q, q), ref_of(m, r2d, r2g, ab), p.far[ab])

    def y2(m, ab):
        q = p.height(m) // 8
        ref = g_ref(m, p.core, p.sub_at(m, ab, p.keep[ab]) + p.quarter * q, q)
        return copy(m, Y2 + ab, ref, ref, p.far[ab])

    def y1(m, ab):
        ref = g_ref(m, p.core, p.sub_at(m, ab, p.keep[ab]), p.height(m) // 4)
        return copy(m, Y1 + ab, ref, ref, p.near[ab])

    def y0(m):
        ref = g_ref(m, p.core, 0, p.height(m))
        return copy(m, Y0, ref, ref, p.other_core)

    def out(m):
        is_down, i, _ = ORDER[m]
        if is_down:
            return pltpu.make_async_copy(gd1, done_d, store.at[m])
        return pltpu.make_async_copy(gg1.at[i], done_g.at[i], store.at[m])

    def out_quarter(m, ab):
        to = own_d.at[ab] if ORDER[m][0] else own_g.at[ORDER[m][1], ab]
        return pltpu.make_async_copy(ref_of(m, r2d, r2g, ab), to, quarters.at[m - 3, ab])

    def c0(m, parts=(0, 1)):
        size = p.height(m) // 2
        for ab in parts:
            s0(m, ab).wait_recv()
            r0 = part(ref_of(m, r0d, r0g), ab * size, size)
            r0[...] = added(r0, g_ref(m, p.core, ab * size, size))
            x1(m, ab).start()
        for ab in parts:
            s0(m, ab).wait_send()
        if ORDER[m][2] and 1 in parts:
            pl.semaphore_signal(credit.at[m], inc=1, device_id={"dp": p.other_core}, device_id_type=MESH)

    def c0a(m):
        c0(m, (0,))

    def c0b(m):
        c0(m, (1,))

    def c1(m):
        for ab in range(2):
            x1(m, ab).wait_recv()
            r1 = ref_of(m, r1d, r1g, ab)
            r1[...] = added(r1, part(ref_of(m, r0d, r0g), p.sub_at(m, ab, p.keep[ab]), p.height(m) // 4))
            x2(m, ab).start()

    def c2(m):
        q = p.height(m) // 8
        for ab in range(2):
            x2(m, ab).wait_recv()
            if ORDER[m][2]:
                to = g_ref(m, p.core, p.sub_at(m, ab, p.keep[ab]) + p.quarter * q, q)
            else:
                to = ref_of(m, r2d, r2g, ab)
            to[...] = added(part(ref_of(m, r1d, r1g, ab), p.quarter * q, q), ref_of(m, r2d, r2g, ab))
            if ORDER[m][2]:
                y2(m, ab).start()
            else:
                out_quarter(m, ab).start()

    def c3(m):
        for ab in range(2):
            y2(m, ab).wait_recv()
            y1(m, ab).start()

    def c4(m):
        for ab in range(2):
            y1(m, ab).wait_recv()
        pl.semaphore_wait(credit.at[m], 1)
        y0(m).start()

    def c5(m):
        y0(m).wait_recv()
        out(m).start()

    def finish(m):
        for ab in range(2):
            for c in (x1, x2, y2, y1) if ORDER[m][2] else (x1, x2):
                c(m, ab).wait_send()
        if ORDER[m][2]:
            y0(m).wait_send()
            out(m).wait()
        else:
            for ab in range(2):
                out_quarter(m, ab).wait()

    def run(step, table):
        for when, todo in table.items():

            @pl.when(step == when)
            def _():
                for what, m in todo:
                    what(m)

    local = {
        "dy": pltpu.make_async_copy(dy, dh, load.at[0]),
        "wd0": pltpu.make_async_copy(wd.at[0], wdv.at[0], load.at[2]),
        "wg1": pltpu.make_async_copy(wg.at[1], wgu1.at[0], load.at[3]),
        "wu1": pltpu.make_async_copy(wu.at[1], wgu1.at[1], load.at[4]),
        "wd1": pltpu.make_async_copy(wd.at[1], wdv.at[1], load.at[5]),
        "mid0": pltpu.make_async_copy(mid0t, midt, load.at[6]),
    }
    xs = [pltpu.make_async_copy(x.at[pl.ds(i, n), :], hv.at[pl.ds(i, n), :], load.at[7 + k]) for k, (i, n) in enumerate(((0, fb), (fb, t - fb)))]
    xs[0].start()
    for c in interleaved(wg, wu, 0, wgu0, load.at[1]):
        c.start()
    local["wd0"].start()
    xs[1].start()
    for name in ("dy", "wd1", "wg1", "wu1"):
        local[name].start()
    p.greet()

    def middle_out(step):
        return pltpu.make_async_copy(midt_out, mid0t.at[:, pl.ds(pl.multiple_of(step * fb, fb), fb)], mid_store)

    def forward(step, carry):
        rows = pl.ds(pl.multiple_of(step * fb, fb), fb)

        @pl.when(step == 0)
        def _():
            xs[0].wait()
            pltpu.make_async_copy(wgu0, wgu0, load.at[1]).wait()

        @pl.when(step == 1)
        def _():
            xs[1].wait()

        @pl.when(step >= 1)
        def _():
            middle_out(step - 1).wait()

        h = hv[rows, :]
        a = normed(h)
        av[rows, :] = a
        for j in range(blocks):
            to = slice(j * LANES, (j + 1) * LANES)
            both = dot(a, wgu0[:, 2 * j * LANES : 2 * (j + 1) * LANES])
            gate, up = both[:, :LANES], both[:, LANES:]
            mid = (gate * jax.nn.sigmoid(gate) * up).astype(BF16)
            mid0[:, to] = mid
            midt_out[to, :] = mid.T

        middle_out(step).start()

        @pl.when(step == 0)
        def _():
            local["wd0"].wait()

        h = h + dot(mid0[...], wdv[0]).astype(BF16)
        hv[rows, :] = h
        a = normed(h)
        at[:, rows] = a.T

        @pl.when(step == 0)
        def _():
            for name in ("dy", "wd1", "wg1", "wu1"):
                local[name].wait()

        by_h = dh[rows, :]
        for pair, width in pairs(blocks):
            to = slice(pair * LANES, (pair + width) * LANES)
            dp = dot_t(by_h, wdv[1, to, :]).astype(BF16).astype(F32)
            gate, up = dot(a, wgu1[0, :, to]), dot(a, wgu1[1, :, to])
            silu, dg, du = backward_of_product(gate, up, dp)
            midt[to, rows] = (silu * up).astype(BF16).T
            dgu[0, rows, to], dgu[1, rows, to] = dg, du
        return carry

    lax.fori_loop(0, t // fb, forward, 0)
    middle_out(t // fb - 1).wait()

    def down_grad(m, gd, table):
        def body(step, carry):
            which = jnp.where(step < 2, 1 - p.core, p.core)
            rows = pl.ds(pl.multiple_of((step % 2) * (ff // 2), 16), ff // 2)
            gd[which, rows, :] = dot(midt[rows, :], dh[:, pl.ds(pl.multiple_of(which * half, half), half)]).astype(BF16)
            for ab in range(2):

                @pl.when(step == ab)
                def _():
                    s0(m, ab).start()

            run(step, table)
            return carry

        lax.fori_loop(0, 4, body, 0)

    def other_grads(m, gg, table):
        def body(step, carry):
            which = jnp.where(step % 2 == 0, 1 - p.core, p.core)
            rows = pl.ds(pl.multiple_of(which * half, half), half)
            gg[step // 2, rows, :] = dot(at[rows, :], dgu[step // 2]).astype(BF16)
            for n in range(2):

                @pl.when(step == 2 * n)
                def _():
                    for ab in range(2):
                        s0(m + n, ab).start()

            run(step, table)
            return carry

        lax.fori_loop(0, 4, body, 0)

    pl.semaphore_wait(pltpu.get_barrier_semaphore(), 3)
    down_grad(0, gd1, {2: [(c0a, 0)], 3: [(c0b, 0)]})
    local["mid0"].start()
    other_grads(1, gg1, {1: [(c1, 0), (c0, 1)], 3: [(c2, 0)]})

    def states_grad(step, carry):
        rows = pl.ds(pl.multiple_of(step * bt, bt), bt)
        by_a = dot_t(dgu[0, rows, :], wgu1[0]).astype(BF16) + dot_t(dgu[1, rows, :], wgu1[1]).astype(BF16)
        by_a = by_a.astype(F32)
        wide = hv[rows, :].astype(F32)
        scale = lax.rsqrt(jnp.mean(wide * wide, -1, keepdims=True) + 1e-6)
        along = jnp.mean(by_a * wide, -1, keepdims=True) * (scale * scale * scale)
        dh[rows, :] = dh[rows, :] + (by_a * scale - wide * along).astype(BF16)
        run(step, {0: [(c0, 2)], 3: [(c1, 1)], 6: [(c1, 2)]})
        return carry

    lax.fori_loop(0, t // bt, states_grad, 0)

    local["mid0"].wait()
    down_grad(3, gd0, {1: [(c3, 0)], 2: [(c2, 1), (c0a, 3)], 3: [(c0b, 3)]})

    def layer_back(step, carry):
        rows = pl.ds(pl.multiple_of(step * bt, bt), bt)
        a, by_h = av[rows, :], dh[rows, :]
        at[:, rows] = a.T
        for pair, width in pairs(blocks):
            dp2 = dot_t(by_h, wdv[0, pair * LANES : (pair + width) * LANES, :]).astype(BF16).astype(F32)
            for j in range(pair, pair + width):
                to = slice(j * LANES, (j + 1) * LANES)
                both = dot(a, wgu0[:, 2 * j * LANES : 2 * (j + 1) * LANES])
                _, dg, du = backward_of_product(both[:, :LANES], both[:, LANES:], dp2[:, (j - pair) * LANES : (j - pair + 1) * LANES])
                dgu[0, rows, to], dgu[1, rows, to] = dg, du
        run(step, {0: [(c2, 2)], 2: [(c4, 0)], 4: [(c5, 0), (c3, 1)], 6: [(c1, 3)], 7: [(c3, 2)]})
        return carry

    lax.fori_loop(0, t // bt, layer_back, 0)
    other_grads(4, gg0, {1: [(c4, 1), (c0, 4)], 2: [(c2, 3), (c5, 1)], 3: [(c0, 5)]})
    for what, m in [(c4, 2), (c1, 4), (c5, 2), (c1, 5), (c2, 4), (c2, 5)]:
        what(m)
    for m in range(6):
        finish(m)


def gradients(x, dy, wg, wu, wd, bt=512):
    t, d = dy.shape
    ff = wg.shape[2]
    half = d // 2
    vmem = lambda *s: pltpu.VMEM(s, BF16)
    return pl.pallas_call(
        gradients_kernel,
        in_specs=[HBM] * 5,
        out_specs=[HBM] * 5,
        out_shape=[
            jax.ShapeDtypeStruct(s, BF16) for s in ((2, d, ff), (2, ff, half), (2, 2, half // 8, ff), (2, ff // 8, half), (ff, t))
        ],
        scratch_shapes=[
            vmem(2, d, ff),
            vmem(2, ff, half),
            vmem(2, d, ff),
            vmem(2, ff, half),
            vmem(4, half, ff),
            vmem(2, ff, half),
            vmem(4, 2, half // 4, ff),
            vmem(2, 2, ff // 4, half),
            vmem(4, 2, half // 8, ff),
            vmem(2, 2, ff // 8, half),
            vmem(ff, t),
            vmem(2, t, ff),
            vmem(d, t),
            vmem(t, d),
            vmem(t, d),
            vmem(t, d),
            vmem(d, 2 * ff),
            vmem(2, d, ff),
            vmem(2, ff, d),
            vmem(bt, ff),
            vmem(ff, bt),
            pltpu.SemaphoreType.DMA((9,)),
            pltpu.SemaphoreType.DMA,
            pltpu.SemaphoreType.DMA((3,)),
            pltpu.SemaphoreType.DMA((3, 2)),
            pltpu.SemaphoreType.DMA((6, 11)),
            pltpu.SemaphoreType.DMA((6, 11)),
            pltpu.SemaphoreType.REGULAR((3,)),
        ],
        compiler_params=pltpu.CompilerParams(collective_id=0, has_side_effects=True, vmem_limit_bytes=67043328),
        name="gradients",
    )(x, dy, wg, wu, wd)[:4]


def update_kernel(
    quarter_g, quarter_d, done_g, done_d, wg, wu, wd, mg, mu, md, vg, vu, vd,
    fg, fd, mg_out, mu_out, md_out, vg_out, vu_out, vd_out,
    own_g, own_d, load, quarters, send, recv,
):
    d, ff = wg.shape[1:]
    half = d // 2
    p = Places(d, ff)

    def f_ref(m, half, start, size):
        layer = ORDER[m][2]
        return p.share(m, fd.at[layer], fg.at[layer], half, start, size)

    def copy(m, kind, src, dst, device):
        at = (m - 3, kind - Y2)
        return pltpu.make_async_remote_copy(
            src_ref=src, dst_ref=dst, send_sem=send.at[at], recv_sem=recv.at[at], device_id={"dp": device}, device_id_type=MESH
        )

    def own_quarter(m, ab):
        q = p.height(m) // 8
        return p.core, p.sub_at(m, ab, p.keep[ab]) + p.quarter * q, q

    def summed(m, ab):
        return quarter_d.at[ab] if ORDER[m][0] else quarter_g.at[ORDER[m][1], ab]

    def y2(m, ab):
        ref = f_ref(m, *own_quarter(m, ab))
        return copy(m, Y2 + ab, ref, ref, p.far[ab])

    def mine(m, ab):
        return pltpu.make_async_copy(summed(m, ab), f_ref(m, *own_quarter(m, ab)), quarters.at[m - 3, ab])

    def y1(m, ab):
        ref = f_ref(m, p.core, p.sub_at(m, ab, p.keep[ab]), p.height(m) // 4)
        return copy(m, Y1 + ab, ref, ref, p.near[ab])

    def y0(m, ab):
        ref = f_ref(m, p.core, p.sub_at(m, ab, p.keep[ab]), p.height(m) // 4)
        return copy(m, Y0 + ab, ref, ref, p.other_core)

    def yr(m, ab):
        ref = f_ref(m, p.core, p.sub_at(m, ab, 1 - p.keep[ab]), p.height(m) // 4)
        return copy(m, YR + ab, ref, ref, p.other_core)

    def loads(m):
        is_down, i, layer = ORDER[m]
        w, mom, var = ((wd, md, vd), (wg, mg, vg), (wu, mu, vu))[0 if is_down else 1 + i]
        mom_out, var_out = ((md_out, vd_out), (mg_out, vg_out), (mu_out, vu_out))[0 if is_down else 1 + i]
        rest = [
            pltpu.make_async_copy(mom.at[layer], mom_out.at[layer], load.at[m, 1]),
            pltpu.make_async_copy(var.at[layer], var_out.at[layer], load.at[m, 2]),
        ]
        if layer:
            if is_down:
                rest.append(pltpu.make_async_copy(done_d, fd.at[layer], load.at[m, 3]))
            else:
                rest.append(pltpu.make_async_copy(done_g.at[i], fg.at[layer, i], load.at[m, 3]))
        to = own_d if is_down else own_g.at[i]
        return pltpu.make_async_copy(w.at[layer], to, load.at[m, 0]), rest

    def adamw(m, half_of, ab, which):
        is_down, i, layer = ORDER[m]
        mom, var = ((md_out, vd_out), (mg_out, vg_out), (mu_out, vu_out))[0 if is_down else 1 + i]
        size = p.height(m) // 4
        start = p.sub_at(m, ab, which)
        if is_down:
            at = (pl.ds(pl.multiple_of(start, 16), size), pl.ds(pl.multiple_of(half_of * half, half), half))
            w = own_d[at]
        else:
            at = (pl.ds(pl.multiple_of(half_of * half + start, 16), size), slice(None))
            w = own_g[(i, *at)]
        w = w.astype(F32)
        f = f_ref(m, half_of, start, size)
        g = f[...].astype(F32)
        new_m = 0.9 * mom[(layer, *at)] + 0.1 * g
        new_v = 0.95 * var[(layer, *at)] + 0.05 * g * g
        f[...] = (w - 0.02 * (new_m * lax.rsqrt(new_v + 1e-8) + 0.1 * w)).astype(BF16)
        mom[(layer, *at)] = new_m
        var[(layer, *at)] = new_v

    def c3(m):
        q = p.height(m) // 8
        for ab in range(2):
            y2(m, ab).wait_recv()
            y1(m, ab).start()
        for ab in range(2):
            y0(m, ab).start()

    def c4(m):
        for ab in range(2):
            y1(m, ab).wait_recv()
            yr(m, ab).start()

    def whole(m):
        own, rest = loads(m)
        own.wait()
        for c in rest:
            c.wait()

        def body(n, carry):
            adamw(m, n // 4, (n // 2) % 2, n % 2)
            return carry

        lax.fori_loop(0, 8, body, 0)
        loads(m + 3)[0].start()

    def others_kept(m):
        own, rest = loads(m)
        own.wait()
        for c in rest:
            c.wait()
        for ab in range(2):
            y0(m, ab).wait_recv()
            adamw(m, 1 - p.core, ab, p.keep[ab])

    def the_rest(m):
        for ab in range(2):
            y2(m, ab).wait_send()
            y0(m, ab).wait_send()
            y1(m, ab).wait_send()
            adamw(m, p.core, ab, p.keep[ab])
        for ab in range(2):
            yr(m, ab).wait_send()
            adamw(m, p.core, ab, 1 - p.keep[ab])
        for ab in range(2):
            yr(m, ab).wait_recv()
            adamw(m, 1 - p.core, ab, 1 - p.keep[ab])

    p.greet()
    for m in (3, 4, 5):
        for ab in range(2):
            mine(m, ab).start()
    for m in range(6):
        own, rest = loads(m)
        if m < 3:
            own.start()
        for c in rest:
            c.start()
    pl.semaphore_wait(pltpu.get_barrier_semaphore(), 3)
    for m in (3, 4, 5):
        for ab in range(2):
            mine(m, ab).wait()
            y2(m, ab).start()
    whole(0)
    c3(3)
    whole(1)
    c3(4)
    whole(2)
    c3(5)
    others_kept(3)
    c4(3)
    the_rest(3)
    others_kept(4)
    c4(4)
    the_rest(4)
    others_kept(5)
    c4(5)
    the_rest(5)


def update(weights, m, v, done_g, done_d, own_g, own_d):
    _, d, ff = weights[0].shape
    half = d // 2
    return pl.pallas_call(
        update_kernel,
        in_specs=[HBM] * 13,
        out_specs=[VMEM] * 8,
        out_shape=[pltpu.VMEM((2, 2, d, ff), BF16), pltpu.VMEM((2, 2, ff, half), BF16)] + [pltpu.VMEM(one.shape, F32) for one in (*m, *v)],
        scratch_shapes=[
            pltpu.VMEM((2, d, ff), BF16),
            pltpu.VMEM((ff, d), BF16),
            pltpu.SemaphoreType.DMA((6, 4)),
            pltpu.SemaphoreType.DMA((3, 2)),
            pltpu.SemaphoreType.DMA((3, 8)),
            pltpu.SemaphoreType.DMA((3, 8)),
        ],
        compiler_params=pltpu.CompilerParams(collective_id=1, has_side_effects=True, vmem_limit_bytes=12 * 2**20),
        name="update",
    )(own_g, own_d, done_g, done_d, *weights, *m, *v)


def written_kernel(fg, fd, mg, mu, md, vg, vu, vd, wg_out, wu_out, wd_out, mg_out, mu_out, md_out, vg_out, vu_out, vd_out, sem):
    layers, _, d, ff = fg.shape
    half = d // 2
    copies = [(one, to) for one, to in zip((mg, mu, md, vg, vu, vd), (mg_out, mu_out, md_out, vg_out, vu_out, vd_out), strict=True)]
    for l in range(layers):
        copies += [(fg.at[l, 0], wg_out.at[l]), (fg.at[l, 1], wu_out.at[l])]
        copies += [(fd.at[l, h], wd_out.at[l, :, pl.ds(h * half, half)]) for h in range(2)]
    copies = [pltpu.make_async_copy(a, b, sem.at[n]) for n, (a, b) in enumerate(copies)]
    for c in copies:
        c.start()
    for c in copies:
        c.wait()


def written(weights, values):
    return pl.pallas_call(
        written_kernel,
        in_specs=[VMEM] * 8,
        out_specs=[HBM] * 9,
        out_shape=[jax.ShapeDtypeStruct(w.shape, kind) for kind in (BF16, F32, F32) for w in weights],
        scratch_shapes=[pltpu.SemaphoreType.DMA((14,))],
        compiler_params=pltpu.CompilerParams(vmem_limit_bytes=12 * 2**20),
        name="written",
    )(*(pltpu.with_memory_space_constraint(one, pltpu.VMEM) for one in values))


def solution(mesh):
    def step(x, dy, *arrays):
        weights, m, v = (arrays[i : i + 3] for i in (0, 3, 6))
        summed = gradients(x[0], dy[0], *weights)
        return tuple(written(weights, update(weights, m, v, *summed)))

    return jax.shard_map(
        step,
        mesh=mesh,
        in_specs=(P(("rep", "dp"), None, None),) * 2 + (P(None, None, None),) * 9,
        out_specs=(P("rep", None, None),) * 9,
        check_vma=False,
    )
```

```python
import jax
import jax.numpy as jnp
from jax import lax
from jax.experimental import pallas as pl
from jax.experimental.pallas import tpu as pltpu
from jax.sharding import PartitionSpec as P

HBM = pl.BlockSpec(memory_space=pltpu.HBM)
VMEM = pl.BlockSpec(memory_space=pltpu.VMEM)
LANES = 128
BF16, F32 = jnp.bfloat16, jnp.float32
MESH = pl.DeviceIdType.MESH


def dot(a, b, dims=((1,), (0,))):
    return lax.dot_general(a, b, (dims, ((), ())), preferred_element_type=F32)


def dot_t(a, b):
    return dot(a, b, ((1,), (1,)))


def normed(h):
    wide = h.astype(F32)
    scale = lax.rsqrt(jnp.mean(wide * wide, -1, keepdims=True) + 1e-6)
    return (wide * scale).astype(BF16)


def interleaved(wg, wu, layer, to, sem):
    out = []
    for j in range(wg.shape[2] // LANES):
        for n, w in enumerate((wg, wu)):
            out.append(pltpu.make_async_copy(w.at[layer, :, pl.ds(j * LANES, LANES)], to.at[:, pl.ds((2 * j + n) * LANES, LANES)], sem))
    return out


def pairs(blocks):
    return [(at, min(2, blocks - at)) for at in range(0, blocks, 2)]


def backward_of_product(gate, up, dp):
    s = jax.nn.sigmoid(gate)
    silu = gate * s
    return silu, (dp * up * (s + silu * (1 - s))).astype(BF16), (dp * silu).astype(BF16)


ORDER = ((True, 0, 1), (False, 0, 1), (False, 1, 1), (True, 0, 0), (False, 0, 0), (False, 1, 0))
S0, X1, X2, Y2, Y1, Y0, YR = 0, 4, 6, 8, 10, 12, 14


class Places:
    def __init__(self, tokens_d, ff):
        self.d, self.ff = tokens_d, ff
        index = lax.axis_index("dp")
        self.core, chip = index % 2, index // 2
        chips = lax.axis_size("dp") // 2
        self.quarter = chip % 2
        after, before = (chip + 1) % chips, (chip + chips - 1) % chips
        first = jnp.where(self.quarter == 0, after, before)
        second = jnp.where(self.quarter == 0, before, after)
        self.other_core = chip * 2 + 1 - self.core
        self.near = (first * 2 + self.core, second * 2 + self.core)
        self.far = (self.near[1], self.near[0])
        self.keep = (((chip + 1) % chips) // 2, chip // 2)

    def height(self, m):
        return self.ff if ORDER[m][0] else self.d // 2

    def sub_at(self, m, ab, which):
        sub = self.height(m) // 4
        return (2 * ab + which) * sub

    def share(self, m, down, other, half, start, size):
        if ORDER[m][0]:
            return down.at[half, pl.ds(pl.multiple_of(start, 16), size), :]
        return other.at[ORDER[m][1], pl.ds(pl.multiple_of(half * (self.d // 2) + start, 16), size), :]

    def greet(self):
        barrier = pltpu.get_barrier_semaphore()
        for other in (self.other_core, *self.near):
            pl.semaphore_signal(barrier, inc=1, device_id={"dp": other}, device_id_type=MESH)


def part(ref, start, size):
    return ref.at[pl.ds(pl.multiple_of(start, 16), size), :]


def added(a, b):
    return (a[...].astype(F32) + b[...].astype(F32)).astype(BF16)


def gradients_kernel(
    x, dy, wg, wu, wd,
    done_g, done_d, own_g, own_d, mid0t,
    gg1, gd1, gg0, gd0, r0g, r0d, r1g, r1d, r2g, r2d,
    midt, dgu, at, av, dh, hv, wgu0, wgu1, wdv, mid0, midt_out,
    load, mid_store, store, quarters, send, recv, credit,
):
    t, d = dh.shape
    ff = wdv.shape[1]
    blocks = ff // LANES
    bt, fb = 256, mid0.shape[0]
    half = d // 2
    p = Places(d, ff)

    def g_ref(m, half, start, size):
        return p.share(m, *((gd1, gg1) if ORDER[m][2] else (gd0, gg0)), half, start, size)

    def ref_of(m, down_ref, other_ref, *at):
        is_down, i, layer = ORDER[m]
        i = layer if is_down else 2 * layer + i
        return (down_ref if is_down else other_ref).at[(i, *at)]

    def copy(m, kind, src, dst, device):
        return pltpu.make_async_remote_copy(
            src_ref=src, dst_ref=dst, send_sem=send.at[m, kind], recv_sem=recv.at[m, kind], device_id={"dp": device}, device_id_type=MESH
        )

    def fourth(m, ab, kept):
        which = p.keep[ab] if kept else 1 - p.keep[ab]
        return p.sub_at(m, ab, which), p.height(m) // 4

    def s0(m, ab, kept):
        at = fourth(m, ab, kept)
        return copy(m, S0 + 2 * kept + ab, g_ref(m, 1 - p.core, *at), part(ref_of(m, r0d, r0g), *at), p.other_core)

    def x1(m, ab):
        src = part(ref_of(m, r0d, r0g), p.sub_at(m, ab, 1 - p.keep[ab]), p.height(m) // 4)
        return copy(m, X1 + ab, src, ref_of(m, r1d, r1g, ab), p.near[ab])

    def x2(m, ab):
        q = p.height(m) // 8
        return copy(m, X2 + ab, part(ref_of(m, r1d, r1g, ab), (1 - p.quarter) * q, q), ref_of(m, r2d, r2g, ab), p.far[ab])

    def y2(m, ab):
        q = p.height(m) // 8
        ref = g_ref(m, p.core, p.sub_at(m, ab, p.keep[ab]) + p.quarter * q, q)
        return copy(m, Y2 + ab, ref, ref, p.far[ab])

    def y1(m, ab):
        ref = g_ref(m, p.core, p.sub_at(m, ab, p.keep[ab]), p.height(m) // 4)
        return copy(m, Y1 + ab, ref, ref, p.near[ab])

    def y0(m):
        ref = g_ref(m, p.core, 0, p.height(m))
        return copy(m, Y0, ref, ref, p.other_core)

    def out(m):
        is_down, i, _ = ORDER[m]
        if is_down:
            return pltpu.make_async_copy(gd1, done_d, store.at[m])
        return pltpu.make_async_copy(gg1.at[i], done_g.at[i], store.at[m])

    def out_quarter(m, ab):
        to = own_d.at[ab] if ORDER[m][0] else own_g.at[ORDER[m][1], ab]
        return pltpu.make_async_copy(ref_of(m, r2d, r2g, ab), to, quarters.at[m - 3, ab])

    def pair_sum(m, ab, kept):
        s0(m, ab, kept).wait_recv()
        at = fourth(m, ab, kept)
        r0 = part(ref_of(m, r0d, r0g), *at)
        r0[...] = added(r0, g_ref(m, p.core, *at))

    def c0a(m):
        pair_sum(m, 0, 0)
        x1(m, 0).start()

    def c0b(m):
        pair_sum(m, 1, 0)
        x1(m, 1).start()

    def c0c(m):
        for ab in range(2):
            pair_sum(m, ab, 1)
        for ab in range(2):
            for kept in range(2):
                s0(m, ab, kept).wait_send()
        if ORDER[m][2]:
            pl.semaphore_signal(credit.at[m], inc=1, device_id={"dp": p.other_core}, device_id_type=MESH)

    def c0(m):
        c0a(m)
        c0b(m)
        c0c(m)

    def c1(m):
        for ab in range(2):
            x1(m, ab).wait_recv()
            r1 = ref_of(m, r1d, r1g, ab)
            r1[...] = added(r1, part(ref_of(m, r0d, r0g), p.sub_at(m, ab, p.keep[ab]), p.height(m) // 4))
            x2(m, ab).start()

    def c2(m):
        q = p.height(m) // 8
        for ab in range(2):
            x2(m, ab).wait_recv()
            if ORDER[m][2]:
                to = g_ref(m, p.core, p.sub_at(m, ab, p.keep[ab]) + p.quarter * q, q)
            else:
                to = ref_of(m, r2d, r2g, ab)
            to[...] = added(part(ref_of(m, r1d, r1g, ab), p.quarter * q, q), ref_of(m, r2d, r2g, ab))
            if ORDER[m][2]:
                y2(m, ab).start()
            else:
                out_quarter(m, ab).start()

    def c3(m):
        for ab in range(2):
            y2(m, ab).wait_recv()
            y1(m, ab).start()

    def c4(m):
        for ab in range(2):
            y1(m, ab).wait_recv()
        pl.semaphore_wait(credit.at[m], 1)
        y0(m).start()

    def c5(m):
        y0(m).wait_recv()
        out(m).start()

    def finish(m):
        for ab in range(2):
            for c in (x1, x2, y2, y1) if ORDER[m][2] else (x1, x2):
                c(m, ab).wait_send()
        if ORDER[m][2]:
            y0(m).wait_send()
            out(m).wait()
        else:
            for ab in range(2):
                out_quarter(m, ab).wait()

    def run(step, table):
        for when, todo in table.items():

            @pl.when(step == when)
            def _():
                for what, m in todo:
                    what(m)

    local = {
        "dy": pltpu.make_async_copy(dy, dh, load.at[0]),
        "wd0": pltpu.make_async_copy(wd.at[0], wdv.at[0], load.at[2]),
        "wg1": pltpu.make_async_copy(wg.at[1], wgu1.at[0], load.at[3]),
        "wu1": pltpu.make_async_copy(wu.at[1], wgu1.at[1], load.at[4]),
        "wd1": pltpu.make_async_copy(wd.at[1], wdv.at[1], load.at[5]),
        "mid0": pltpu.make_async_copy(mid0t, midt, load.at[6]),
    }
    xs = [pltpu.make_async_copy(x.at[pl.ds(i, n), :], hv.at[pl.ds(i, n), :], load.at[7 + k]) for k, (i, n) in enumerate(((0, fb), (fb, t - fb)))]
    xs[0].start()
    for c in interleaved(wg, wu, 0, wgu0, load.at[1]):
        c.start()
    local["wd0"].start()
    xs[1].start()
    for name in ("dy", "wd1", "wg1", "wu1"):
        local[name].start()
    p.greet()

    def middle_out(step):
        return pltpu.make_async_copy(midt_out, mid0t.at[:, pl.ds(pl.multiple_of(step * fb, fb), fb)], mid_store)

    def forward(step, carry):
        rows = pl.ds(pl.multiple_of(step * fb, fb), fb)

        @pl.when(step == 0)
        def _():
            xs[0].wait()
            pltpu.make_async_copy(wgu0, wgu0, load.at[1]).wait()

        @pl.when(step == 1)
        def _():
            xs[1].wait()

        @pl.when(step >= 1)
        def _():
            middle_out(step - 1).wait()

        h = hv[rows, :]
        a = normed(h)
        av[rows, :] = a
        for j in range(blocks):
            to = slice(j * LANES, (j + 1) * LANES)
            both = dot(a, wgu0[:, 2 * j * LANES : 2 * (j + 1) * LANES])
            gate, up = both[:, :LANES], both[:, LANES:]
            mid = (gate * jax.nn.sigmoid(gate) * up).astype(BF16)
            mid0[:, to] = mid
            midt_out[to, :] = mid.T

        middle_out(step).start()

        @pl.when(step == 0)
        def _():
            for name in ("wd0", "dy", "wd1"):
                local[name].wait()

        h = h + dot(mid0[...], wdv[0]).astype(BF16)
        by_h = dh[rows, :]
        for pair, width in pairs(blocks):
            to = slice(pair * LANES, (pair + width) * LANES)
            dgu[1, rows, to] = dot_t(by_h, wdv[1, to, :]).astype(BF16)
        hv[rows, :] = h
        a = normed(h)
        at[:, rows] = a.T

        @pl.when(step == 0)
        def _():
            for name in ("wg1", "wu1"):
                local[name].wait()

        for pair, width in pairs(blocks):
            to = slice(pair * LANES, (pair + width) * LANES)
            dp = dgu[1, rows, to].astype(F32)
            gate, up = dot(a, wgu1[0, :, to]), dot(a, wgu1[1, :, to])
            silu, dg, du = backward_of_product(gate, up, dp)
            midt[to, rows] = (silu * up).astype(BF16).T
            dgu[0, rows, to], dgu[1, rows, to] = dg, du
        return carry

    lax.fori_loop(0, t // fb, forward, 0)
    middle_out(t // fb - 1).wait()

    def down_grad(m, gd, table):
        sub = ff // 4

        def body(step, carry):
            kept, own, ab = step // 4, (step % 4) // 2, step % 2
            which = jnp.where(own == 0, 1 - p.core, p.core)
            keep = jnp.where(ab == 0, p.keep[0], p.keep[1])
            at = 2 * ab + jnp.where(kept == 0, 1 - keep, keep)
            rows = pl.ds(pl.multiple_of(at * sub, 16), sub)
            gd[which, rows, :] = dot(midt[rows, :], dh[:, pl.ds(pl.multiple_of(which * half, half), half)]).astype(BF16)
            for k in range(2):
                for n in range(2):

                    @pl.when(step == 4 * k + n)
                    def _():
                        s0(m, n, k).start()

            run(step, table)
            return carry

        lax.fori_loop(0, 8, body, 0)

    def other_grads(m, gg, table):
        def body(step, carry):
            which = jnp.where(step % 2 == 0, 1 - p.core, p.core)
            rows = pl.ds(pl.multiple_of(which * half, half), half)
            gg[step // 2, rows, :] = dot(at[rows, :], dgu[step // 2]).astype(BF16)
            for n in range(2):

                @pl.when(step == 2 * n)
                def _():
                    for kept in range(2):
                        for ab in range(2):
                            s0(m + n, ab, kept).start()

            run(step, table)
            return carry

        lax.fori_loop(0, 4, body, 0)

    pl.semaphore_wait(pltpu.get_barrier_semaphore(), 3)
    down_grad(0, gd1, {3: [(c0a, 0)], 4: [(c0b, 0)]})
    local["mid0"].start()
    other_grads(1, gg1, {0: [(c0c, 0)], 1: [(c1, 0), (c0, 1)], 3: [(c2, 0)]})

    def states_grad(step, carry):
        rows = pl.ds(pl.multiple_of(step * bt, bt), bt)
        by_a = dot_t(dgu[0, rows, :], wgu1[0]).astype(BF16) + dot_t(dgu[1, rows, :], wgu1[1]).astype(BF16)
        by_a = by_a.astype(F32)
        wide = hv[rows, :].astype(F32)
        scale = lax.rsqrt(jnp.mean(wide * wide, -1, keepdims=True) + 1e-6)
        along = jnp.mean(by_a * wide, -1, keepdims=True) * (scale * scale * scale)
        dh[rows, :] = dh[rows, :] + (by_a * scale - wide * along).astype(BF16)
        run(step, {0: [(c0, 2)], 3: [(c1, 1)], 6: [(c1, 2)]})
        return carry

    lax.fori_loop(0, t // bt, states_grad, 0)

    local["mid0"].wait()
    down_grad(3, gd0, {1: [(c3, 0)], 3: [(c2, 1), (c0a, 3)], 4: [(c0b, 3)]})

    def layer_back(step, carry):
        rows = pl.ds(pl.multiple_of(step * bt, bt), bt)
        a, by_h = av[rows, :], dh[rows, :]
        at[:, rows] = a.T
        for pair, width in pairs(blocks):
            dp2 = dot_t(by_h, wdv[0, pair * LANES : (pair + width) * LANES, :]).astype(BF16).astype(F32)
            for j in range(pair, pair + width):
                to = slice(j * LANES, (j + 1) * LANES)
                both = dot(a, wgu0[:, 2 * j * LANES : 2 * (j + 1) * LANES])
                _, dg, du = backward_of_product(both[:, :LANES], both[:, LANES:], dp2[:, (j - pair) * LANES : (j - pair + 1) * LANES])
                dgu[0, rows, to], dgu[1, rows, to] = dg, du
        run(step, {0: [(c0c, 3), (c2, 2)], 2: [(c4, 0)], 4: [(c5, 0), (c3, 1)], 6: [(c1, 3)], 7: [(c3, 2)]})
        return carry

    lax.fori_loop(0, t // bt, layer_back, 0)
    other_grads(4, gg0, {1: [(c4, 1), (c0, 4)], 2: [(c2, 3), (c5, 1)], 3: [(c0, 5)]})
    for what, m in [(c4, 2), (c1, 4), (c5, 2), (c1, 5), (c2, 4), (c2, 5)]:
        what(m)
    for m in range(6):
        finish(m)


def gradients(x, dy, wg, wu, wd, bt=512):
    t, d = dy.shape
    ff = wg.shape[2]
    half = d // 2
    vmem = lambda *s: pltpu.VMEM(s, BF16)
    return pl.pallas_call(
        gradients_kernel,
        in_specs=[HBM] * 5,
        out_specs=[HBM] * 5,
        out_shape=[
            jax.ShapeDtypeStruct(s, BF16) for s in ((2, d, ff), (2, ff, half), (2, 2, half // 8, ff), (2, ff // 8, half), (ff, t))
        ],
        scratch_shapes=[
            vmem(2, d, ff),
            vmem(2, ff, half),
            vmem(2, d, ff),
            vmem(2, ff, half),
            vmem(4, half, ff),
            vmem(2, ff, half),
            vmem(4, 2, half // 4, ff),
            vmem(2, 2, ff // 4, half),
            vmem(4, 2, half // 8, ff),
            vmem(2, 2, ff // 8, half),
            vmem(ff, t),
            vmem(2, t, ff),
            vmem(d, t),
            vmem(t, d),
            vmem(t, d),
            vmem(t, d),
            vmem(d, 2 * ff),
            vmem(2, d, ff),
            vmem(2, ff, d),
            vmem(bt, ff),
            vmem(ff, bt),
            pltpu.SemaphoreType.DMA((9,)),
            pltpu.SemaphoreType.DMA,
            pltpu.SemaphoreType.DMA((3,)),
            pltpu.SemaphoreType.DMA((3, 2)),
            pltpu.SemaphoreType.DMA((6, 13)),
            pltpu.SemaphoreType.DMA((6, 13)),
            pltpu.SemaphoreType.REGULAR((3,)),
        ],
        compiler_params=pltpu.CompilerParams(collective_id=0, has_side_effects=True, vmem_limit_bytes=67043328),
        name="gradients",
    )(x, dy, wg, wu, wd)[:4]


def update_kernel(
    quarter_g, quarter_d, done_g, done_d, wg, wu, wd, mg, mu, md, vg, vu, vd,
    fg, fd, mg_out, mu_out, md_out, vg_out, vu_out, vd_out,
    own_g, own_d, load, quarters, send, recv,
):
    d, ff = wg.shape[1:]
    half = d // 2
    p = Places(d, ff)

    def f_ref(m, half, start, size):
        layer = ORDER[m][2]
        return p.share(m, fd.at[layer], fg.at[layer], half, start, size)

    def copy(m, kind, src, dst, device):
        at = (m - 3, kind - Y2)
        return pltpu.make_async_remote_copy(
            src_ref=src, dst_ref=dst, send_sem=send.at[at], recv_sem=recv.at[at], device_id={"dp": device}, device_id_type=MESH
        )

    def own_quarter(m, ab):
        q = p.height(m) // 8
        return p.core, p.sub_at(m, ab, p.keep[ab]) + p.quarter * q, q

    def summed(m, ab):
        return quarter_d.at[ab] if ORDER[m][0] else quarter_g.at[ORDER[m][1], ab]

    def y2(m, ab):
        ref = f_ref(m, *own_quarter(m, ab))
        return copy(m, Y2 + ab, ref, ref, p.far[ab])

    def mine(m, ab):
        return pltpu.make_async_copy(summed(m, ab), f_ref(m, *own_quarter(m, ab)), quarters.at[m - 3, ab])

    def y1(m, ab):
        ref = f_ref(m, p.core, p.sub_at(m, ab, p.keep[ab]), p.height(m) // 4)
        return copy(m, Y1 + ab, ref, ref, p.near[ab])

    def y0(m, ab):
        ref = f_ref(m, p.core, p.sub_at(m, ab, p.keep[ab]), p.height(m) // 4)
        return copy(m, Y0 + ab, ref, ref, p.other_core)

    def yr(m, ab):
        ref = f_ref(m, p.core, p.sub_at(m, ab, 1 - p.keep[ab]), p.height(m) // 4)
        return copy(m, YR + ab, ref, ref, p.other_core)

    def loads(m):
        is_down, i, layer = ORDER[m]
        w, mom, var = ((wd, md, vd), (wg, mg, vg), (wu, mu, vu))[0 if is_down else 1 + i]
        mom_out, var_out = ((md_out, vd_out), (mg_out, vg_out), (mu_out, vu_out))[0 if is_down else 1 + i]
        rest = [
            pltpu.make_async_copy(mom.at[layer], mom_out.at[layer], load.at[m, 1]),
            pltpu.make_async_copy(var.at[layer], var_out.at[layer], load.at[m, 2]),
        ]
        if layer:
            if is_down:
                rest.append(pltpu.make_async_copy(done_d, fd.at[layer], load.at[m, 3]))
            else:
                rest.append(pltpu.make_async_copy(done_g.at[i], fg.at[layer, i], load.at[m, 3]))
        to = own_d if is_down else own_g.at[i]
        return pltpu.make_async_copy(w.at[layer], to, load.at[m, 0]), rest

    def adamw(m, half_of, ab, which):
        is_down, i, layer = ORDER[m]
        mom, var = ((md_out, vd_out), (mg_out, vg_out), (mu_out, vu_out))[0 if is_down else 1 + i]
        size = p.height(m) // 4
        start = p.sub_at(m, ab, which)
        if is_down:
            at = (pl.ds(pl.multiple_of(start, 16), size), pl.ds(pl.multiple_of(half_of * half, half), half))
            w = own_d[at]
        else:
            at = (pl.ds(pl.multiple_of(half_of * half + start, 16), size), slice(None))
            w = own_g[(i, *at)]
        w = w.astype(F32)
        f = f_ref(m, half_of, start, size)
        g = f[...].astype(F32)
        new_m = 0.9 * mom[(layer, *at)] + 0.1 * g
        new_v = 0.95 * var[(layer, *at)] + 0.05 * g * g
        f[...] = (w - 0.02 * (new_m * lax.rsqrt(new_v + 1e-8) + 0.1 * w)).astype(BF16)
        mom[(layer, *at)] = new_m
        var[(layer, *at)] = new_v

    def c3(m):
        q = p.height(m) // 8
        for ab in range(2):
            y2(m, ab).wait_recv()
            y1(m, ab).start()
        for ab in range(2):
            y0(m, ab).start()

    def c4(m):
        for ab in range(2):
            y1(m, ab).wait_recv()
            yr(m, ab).start()

    def whole(m):
        own, rest = loads(m)
        own.wait()
        for c in rest:
            c.wait()

        def body(n, carry):
            adamw(m, n // 4, (n // 2) % 2, n % 2)
            return carry

        lax.fori_loop(0, 8, body, 0)
        loads(m + 3)[0].start()

    def others_kept(m):
        own, rest = loads(m)
        own.wait()
        for c in rest:
            c.wait()
        for ab in range(2):
            y0(m, ab).wait_recv()
            adamw(m, 1 - p.core, ab, p.keep[ab])

    def the_rest(m):
        for ab in range(2):
            y2(m, ab).wait_send()
            y0(m, ab).wait_send()
            y1(m, ab).wait_send()
            adamw(m, p.core, ab, p.keep[ab])
        for ab in range(2):
            yr(m, ab).wait_send()
            adamw(m, p.core, ab, 1 - p.keep[ab])
        for ab in range(2):
            yr(m, ab).wait_recv()
            adamw(m, 1 - p.core, ab, 1 - p.keep[ab])

    p.greet()
    for m in (3, 4, 5):
        for ab in range(2):
            mine(m, ab).start()
    for m in range(6):
        own, rest = loads(m)
        if m < 3:
            own.start()
        for c in rest:
            c.start()
    pl.semaphore_wait(pltpu.get_barrier_semaphore(), 3)
    for m in (3, 4, 5):
        for ab in range(2):
            mine(m, ab).wait()
            y2(m, ab).start()
    whole(0)
    c3(3)
    whole(1)
    c3(4)
    whole(2)
    c3(5)
    others_kept(3)
    c4(3)
    the_rest(3)
    others_kept(4)
    c4(4)
    the_rest(4)
    others_kept(5)
    c4(5)
    the_rest(5)


def update(weights, m, v, done_g, done_d, own_g, own_d):
    _, d, ff = weights[0].shape
    half = d // 2
    return pl.pallas_call(
        update_kernel,
        in_specs=[HBM] * 13,
        out_specs=[VMEM] * 8,
        out_shape=[pltpu.VMEM((2, 2, d, ff), BF16), pltpu.VMEM((2, 2, ff, half), BF16)] + [pltpu.VMEM(one.shape, F32) for one in (*m, *v)],
        scratch_shapes=[
            pltpu.VMEM((2, d, ff), BF16),
            pltpu.VMEM((ff, d), BF16),
            pltpu.SemaphoreType.DMA((6, 4)),
            pltpu.SemaphoreType.DMA((3, 2)),
            pltpu.SemaphoreType.DMA((3, 8)),
            pltpu.SemaphoreType.DMA((3, 8)),
        ],
        compiler_params=pltpu.CompilerParams(collective_id=1, has_side_effects=True, vmem_limit_bytes=12 * 2**20),
        name="update",
    )(own_g, own_d, done_g, done_d, *weights, *m, *v)


def written_kernel(fg, fd, mg, mu, md, vg, vu, vd, wg_out, wu_out, wd_out, mg_out, mu_out, md_out, vg_out, vu_out, vd_out, sem):
    layers, _, d, ff = fg.shape
    half = d // 2
    copies = [(one, to) for one, to in zip((mg, mu, md, vg, vu, vd), (mg_out, mu_out, md_out, vg_out, vu_out, vd_out), strict=True)]
    for l in range(layers):
        copies += [(fg.at[l, 0], wg_out.at[l]), (fg.at[l, 1], wu_out.at[l])]
        copies += [(fd.at[l, h], wd_out.at[l, :, pl.ds(h * half, half)]) for h in range(2)]
    copies = [pltpu.make_async_copy(a, b, sem.at[n]) for n, (a, b) in enumerate(copies)]
    for c in copies:
        c.start()
    for c in copies:
        c.wait()


def written(weights, values):
    return pl.pallas_call(
        written_kernel,
        in_specs=[VMEM] * 8,
        out_specs=[HBM] * 9,
        out_shape=[jax.ShapeDtypeStruct(w.shape, kind) for kind in (BF16, F32, F32) for w in weights],
        scratch_shapes=[pltpu.SemaphoreType.DMA((14,))],
        compiler_params=pltpu.CompilerParams(vmem_limit_bytes=12 * 2**20),
        name="written",
    )(*(pltpu.with_memory_space_constraint(one, pltpu.VMEM) for one in values))


def solution(mesh):
    def step(x, dy, *arrays):
        weights, m, v = (arrays[i : i + 3] for i in (0, 3, 6))
        summed = gradients(x[0], dy[0], *weights)
        return tuple(written(weights, update(weights, m, v, *summed)))

    return jax.shard_map(
        step,
        mesh=mesh,
        in_specs=(P(("rep", "dp"), None, None),) * 2 + (P(None, None, None),) * 9,
        out_specs=(P("rep", None, None),) * 9,
        check_vma=False,
    )
```

```python
import jax
import jax.numpy as jnp
from jax import lax
from jax.experimental import pallas as pl
from jax.experimental.pallas import tpu as pltpu
from jax.sharding import PartitionSpec as P

HBM = pl.BlockSpec(memory_space=pltpu.HBM)
VMEM = pl.BlockSpec(memory_space=pltpu.VMEM)
LANES = 128
BF16, F32 = jnp.bfloat16, jnp.float32
MESH = pl.DeviceIdType.MESH


def dot(a, b, dims=((1,), (0,))):
    return lax.dot_general(a, b, (dims, ((), ())), preferred_element_type=F32)


def dot_t(a, b):
    return dot(a, b, ((1,), (1,)))


def normed(h):
    wide = h.astype(F32)
    scale = lax.rsqrt(jnp.mean(wide * wide, -1, keepdims=True) + 1e-6)
    return (wide * scale).astype(BF16)


def interleaved(wg, wu, layer, to, sem):
    out = []
    for j in range(wg.shape[2] // LANES):
        for n, w in enumerate((wg, wu)):
            out.append(pltpu.make_async_copy(w.at[layer, :, pl.ds(j * LANES, LANES)], to.at[:, pl.ds((2 * j + n) * LANES, LANES)], sem))
    return out


def pairs(blocks):
    return [(at, min(2, blocks - at)) for at in range(0, blocks, 2)]


def backward_of_product(gate, up, dp):
    s = jax.nn.sigmoid(gate)
    silu = gate * s
    return silu, (dp * up * (s + silu * (1 - s))).astype(BF16), (dp * silu).astype(BF16)


ORDER = ((True, 0, 1), (False, 0, 1), (False, 1, 1), (True, 0, 0), (False, 0, 0), (False, 1, 0))
S0, X1, X2, Y2, Y1, Y0, YR = 0, 4, 6, 8, 10, 12, 14


class Places:
    def __init__(self, tokens_d, ff):
        self.d, self.ff = tokens_d, ff
        index = lax.axis_index("dp")
        self.core, chip = index % 2, index // 2
        chips = lax.axis_size("dp") // 2
        self.quarter = chip % 2
        after, before = (chip + 1) % chips, (chip + chips - 1) % chips
        first = jnp.where(self.quarter == 0, after, before)
        second = jnp.where(self.quarter == 0, before, after)
        self.other_core = chip * 2 + 1 - self.core
        self.near = (first * 2 + self.core, second * 2 + self.core)
        self.far = (self.near[1], self.near[0])
        self.keep = (((chip + 1) % chips) // 2, chip // 2)

    def height(self, m):
        return self.ff if ORDER[m][0] else self.d // 2

    def sub_at(self, m, ab, which):
        sub = self.height(m) // 4
        return (2 * ab + which) * sub

    def share(self, m, down, other, half, start, size):
        if ORDER[m][0]:
            return down.at[half, pl.ds(pl.multiple_of(start, 16), size), :]
        return other.at[ORDER[m][1], pl.ds(pl.multiple_of(half * (self.d // 2) + start, 16), size), :]

    def greet(self):
        barrier = pltpu.get_barrier_semaphore()
        for other in (self.other_core, *self.near):
            pl.semaphore_signal(barrier, inc=1, device_id={"dp": other}, device_id_type=MESH)


def part(ref, start, size):
    return ref.at[pl.ds(pl.multiple_of(start, 16), size), :]


def added(a, b):
    return (a[...].astype(F32) + b[...].astype(F32)).astype(BF16)


def gradients_kernel(
    x, dy, wg, wu, wd,
    done_g, done_d, own_g, own_d, mid0t,
    gg1, gd1, gg0, gd0, r0g, r0d, r1g, r1d, r2g, r2d,
    midt, dgu, at, av, dh, hv, wgu0, wgu1, wdv, mid0, midt_out,
    load, mid_store, store, quarters, send, recv, credit,
):
    t, d = dh.shape
    ff = wdv.shape[1]
    blocks = ff // LANES
    bt, fb = 256, mid0.shape[0]
    half = d // 2
    p = Places(d, ff)

    def g_ref(m, half, start, size):
        return p.share(m, *((gd1, gg1) if ORDER[m][2] else (gd0, gg0)), half, start, size)

    def ref_of(m, down_ref, other_ref, *at):
        is_down, i, layer = ORDER[m]
        i = layer if is_down else 2 * layer + i
        return (down_ref if is_down else other_ref).at[(i, *at)]

    def copy(m, kind, src, dst, device):
        return pltpu.make_async_remote_copy(
            src_ref=src, dst_ref=dst, send_sem=send.at[m, kind], recv_sem=recv.at[m, kind], device_id={"dp": device}, device_id_type=MESH
        )

    def fourth(m, ab, kept):
        which = p.keep[ab] if kept else 1 - p.keep[ab]
        return p.sub_at(m, ab, which), p.height(m) // 4

    def s0(m, ab, kept):
        at = fourth(m, ab, kept)
        return copy(m, S0 + 2 * kept + ab, g_ref(m, 1 - p.core, *at), part(ref_of(m, r0d, r0g), *at), p.other_core)

    def x1(m, ab):
        src = part(ref_of(m, r0d, r0g), p.sub_at(m, ab, 1 - p.keep[ab]), p.height(m) // 4)
        return copy(m, X1 + ab, src, ref_of(m, r1d, r1g, ab), p.near[ab])

    def x2(m, ab):
        q = p.height(m) // 8
        return copy(m, X2 + ab, part(ref_of(m, r1d, r1g, ab), (1 - p.quarter) * q, q), ref_of(m, r2d, r2g, ab), p.far[ab])

    def y2(m, ab):
        q = p.height(m) // 8
        ref = g_ref(m, p.core, p.sub_at(m, ab, p.keep[ab]) + p.quarter * q, q)
        return copy(m, Y2 + ab, ref, ref, p.far[ab])

    def y1(m, ab):
        ref = g_ref(m, p.core, p.sub_at(m, ab, p.keep[ab]), p.height(m) // 4)
        return copy(m, Y1 + ab, ref, ref, p.near[ab])

    def y0(m):
        ref = g_ref(m, p.core, 0, p.height(m))
        return copy(m, Y0, ref, ref, p.other_core)

    def out(m):
        is_down, i, _ = ORDER[m]
        if is_down:
            return pltpu.make_async_copy(gd1, done_d, store.at[m])
        return pltpu.make_async_copy(gg1.at[i], done_g.at[i], store.at[m])

    def out_quarter(m, ab):
        to = own_d.at[ab] if ORDER[m][0] else own_g.at[ORDER[m][1], ab]
        return pltpu.make_async_copy(ref_of(m, r2d, r2g, ab), to, quarters.at[m - 3, ab])

    def pair_sum(m, ab, kept):
        s0(m, ab, kept).wait_recv()
        at = fourth(m, ab, kept)
        r0 = part(ref_of(m, r0d, r0g), *at)
        r0[...] = added(r0, g_ref(m, p.core, *at))

    def c0a(m):
        pair_sum(m, 0, 0)
        x1(m, 0).start()

    def c0b(m):
        pair_sum(m, 1, 0)
        x1(m, 1).start()

    def c0c(m):
        for ab in range(2):
            pair_sum(m, ab, 1)
        for ab in range(2):
            for kept in range(2):
                s0(m, ab, kept).wait_send()
        if ORDER[m][2]:
            pl.semaphore_signal(credit.at[m], inc=1, device_id={"dp": p.other_core}, device_id_type=MESH)

    def c0(m):
        c0a(m)
        c0b(m)
        c0c(m)

    def c1(m):
        for ab in range(2):
            x1(m, ab).wait_recv()
            r1 = ref_of(m, r1d, r1g, ab)
            r1[...] = added(r1, part(ref_of(m, r0d, r0g), p.sub_at(m, ab, p.keep[ab]), p.height(m) // 4))
            x2(m, ab).start()

    def c2(m):
        q = p.height(m) // 8
        for ab in range(2):
            x2(m, ab).wait_recv()
            if ORDER[m][2]:
                to = g_ref(m, p.core, p.sub_at(m, ab, p.keep[ab]) + p.quarter * q, q)
            else:
                to = ref_of(m, r2d, r2g, ab)
            to[...] = added(part(ref_of(m, r1d, r1g, ab), p.quarter * q, q), ref_of(m, r2d, r2g, ab))
            if ORDER[m][2]:
                y2(m, ab).start()
            else:
                out_quarter(m, ab).start()

    def c3(m):
        for ab in range(2):
            y2(m, ab).wait_recv()
            y1(m, ab).start()

    def c4(m):
        for ab in range(2):
            y1(m, ab).wait_recv()
        pl.semaphore_wait(credit.at[m], 1)
        y0(m).start()

    def c5(m):
        y0(m).wait_recv()
        out(m).start()

    def finish(m):
        for ab in range(2):
            for c in (x1, x2, y2, y1) if ORDER[m][2] else (x1, x2):
                c(m, ab).wait_send()
        if ORDER[m][2]:
            y0(m).wait_send()
            out(m).wait()
        else:
            for ab in range(2):
                out_quarter(m, ab).wait()

    def run(step, table):
        for when, todo in table.items():

            @pl.when(step == when)
            def _():
                for what, m in todo:
                    what(m)

    local = {
        "dy": pltpu.make_async_copy(dy, dh, load.at[0]),
        "wd0": pltpu.make_async_copy(wd.at[0], wdv.at[0], load.at[2]),
        "wg1": pltpu.make_async_copy(wg.at[1], wgu1.at[0], load.at[3]),
        "wu1": pltpu.make_async_copy(wu.at[1], wgu1.at[1], load.at[4]),
        "wd1": pltpu.make_async_copy(wd.at[1], wdv.at[1], load.at[5]),
        "mid0": pltpu.make_async_copy(mid0t, midt, load.at[6]),
    }
    xs = [pltpu.make_async_copy(x.at[pl.ds(i, n), :], hv.at[pl.ds(i, n), :], load.at[7 + k]) for k, (i, n) in enumerate(((0, fb), (fb, t - fb)))]
    xs[0].start()
    for c in interleaved(wg, wu, 0, wgu0, load.at[1]):
        c.start()
    local["wd0"].start()
    xs[1].start()
    for name in ("dy", "wd1", "wg1", "wu1"):
        local[name].start()
    p.greet()

    def middle_out(step):
        return pltpu.make_async_copy(midt_out, mid0t.at[:, pl.ds(pl.multiple_of(step * fb, fb), fb)], mid_store)

    def forward(step, carry):
        rows = pl.ds(pl.multiple_of(step * fb, fb), fb)

        @pl.when(step == 0)
        def _():
            xs[0].wait()
            pltpu.make_async_copy(wgu0, wgu0, load.at[1]).wait()

        @pl.when(step == 1)
        def _():
            xs[1].wait()

        @pl.when(step >= 1)
        def _():
            middle_out(step - 1).wait()

        h = hv[rows, :]
        a = normed(h)
        av[rows, :] = a
        for j in range(blocks):
            to = slice(j * LANES, (j + 1) * LANES)
            both = dot(a, wgu0[:, 2 * j * LANES : 2 * (j + 1) * LANES])
            gate, up = both[:, :LANES], both[:, LANES:]
            mid = (gate * jax.nn.sigmoid(gate) * up).astype(BF16)
            mid0[:, to] = mid
            midt_out[to, :] = mid.T

        middle_out(step).start()

        @pl.when(step == 0)
        def _():
            for name in ("wd0", "dy", "wd1"):
                local[name].wait()

        h = h + dot(mid0[...], wdv[0]).astype(BF16)
        by_h = dh[rows, :]
        for pair, width in pairs(blocks):
            to = slice(pair * LANES, (pair + width) * LANES)
            dgu[1, rows, to] = dot_t(by_h, wdv[1, to, :]).astype(BF16)
        hv[rows, :] = h
        a = normed(h)
        at[:, rows] = a.T

        @pl.when(step == 0)
        def _():
            for name in ("wg1", "wu1"):
                local[name].wait()

        for pair, width in pairs(blocks):
            to = slice(pair * LANES, (pair + width) * LANES)
            dp = dgu[1, rows, to].astype(F32)
            gate, up = dot(a, wgu1[0, :, to]), dot(a, wgu1[1, :, to])
            silu, dg, du = backward_of_product(gate, up, dp)
            midt[to, rows] = (silu * up).astype(BF16).T
            dgu[0, rows, to], dgu[1, rows, to] = dg, du
        return carry

    lax.fori_loop(0, t // fb, forward, 0)
    middle_out(t // fb - 1).wait()

    def down_grad(m, gd, table, steps=(0, 8)):
        sub = ff // 4

        def body(step, carry):
            kept, own, ab = step // 4, (step % 4) // 2, step % 2
            which = jnp.where(own == 0, 1 - p.core, p.core)
            keep = jnp.where(ab == 0, p.keep[0], p.keep[1])
            at = 2 * ab + jnp.where(kept == 0, 1 - keep, keep)
            rows = pl.ds(pl.multiple_of(at * sub, 16), sub)
            gd[which, rows, :] = dot(midt[rows, :], dh[:, pl.ds(pl.multiple_of(which * half, half), half)]).astype(BF16)
            for k in range(2):
                for n in range(2):

                    @pl.when(step == 4 * k + n)
                    def _():
                        s0(m, n, k).start()

            run(step, table)
            return carry

        lax.fori_loop(*steps, body, 0)

    def other_grads(m, gg, table, steps=(0, 4)):
        def body(step, carry):
            which = jnp.where(step % 2 == 0, 1 - p.core, p.core)
            rows = pl.ds(pl.multiple_of(which * half, half), half)
            gg[step // 2, rows, :] = dot(at[rows, :], dgu[step // 2]).astype(BF16)
            for n in range(2):

                @pl.when(step == 2 * n)
                def _():
                    for kept in range(2):
                        for ab in range(2):
                            s0(m + n, ab, kept).start()

            run(step, table)
            return carry

        lax.fori_loop(*steps, body, 0)

    pl.semaphore_wait(pltpu.get_barrier_semaphore(), 3)
    down_grad(0, gd1, {3: [(c0a, 0), (c0b, 0)]}, (0, 4))
    other_grads(1, gg1, {1: [(c0a, 1), (c0b, 1)]}, (0, 2))
    down_grad(0, gd1, {}, (4, 8))
    local["mid0"].start()
    other_grads(1, gg1, {2: [(c0c, 0), (c0c, 1), (c1, 0)], 3: [(c0, 2)]}, (2, 4))

    def states_grad(step, carry):
        rows = pl.ds(pl.multiple_of(step * bt, bt), bt)
        by_a = dot_t(dgu[0, rows, :], wgu1[0]).astype(BF16) + dot_t(dgu[1, rows, :], wgu1[1]).astype(BF16)
        by_a = by_a.astype(F32)
        wide = hv[rows, :].astype(F32)
        scale = lax.rsqrt(jnp.mean(wide * wide, -1, keepdims=True) + 1e-6)
        along = jnp.mean(by_a * wide, -1, keepdims=True) * (scale * scale * scale)
        dh[rows, :] = dh[rows, :] + (by_a * scale - wide * along).astype(BF16)
        run(step, {0: [(c1, 1)], 2: [(c2, 0)], 6: [(c1, 2)]})
        return carry

    lax.fori_loop(0, t // bt, states_grad, 0)

    local["mid0"].wait()
    down_grad(3, gd0, {0: [(c2, 1)], 3: [(c3, 0), (c0a, 3)], 4: [(c0b, 3)]})

    def layer_back(step, carry):
        rows = pl.ds(pl.multiple_of(step * bt, bt), bt)
        a, by_h = av[rows, :], dh[rows, :]
        at[:, rows] = a.T
        for pair, width in pairs(blocks):
            dp2 = dot_t(by_h, wdv[0, pair * LANES : (pair + width) * LANES, :]).astype(BF16).astype(F32)
            for j in range(pair, pair + width):
                to = slice(j * LANES, (j + 1) * LANES)
                both = dot(a, wgu0[:, 2 * j * LANES : 2 * (j + 1) * LANES])
                _, dg, du = backward_of_product(both[:, :LANES], both[:, LANES:], dp2[:, (j - pair) * LANES : (j - pair + 1) * LANES])
                dgu[0, rows, to], dgu[1, rows, to] = dg, du
        run(step, {0: [(c0c, 3), (c2, 2)], 1: [(c3, 1)], 3: [(c4, 0)], 5: [(c5, 0)], 6: [(c1, 3)], 7: [(c3, 2)]})
        return carry

    lax.fori_loop(0, t // bt, layer_back, 0)
    other_grads(4, gg0, {1: [(c0, 4), (c4, 1)], 3: [(c0, 5), (c2, 3), (c5, 1)]})
    for what, m in [(c4, 2), (c1, 4), (c5, 2), (c1, 5), (c2, 4), (c2, 5)]:
        what(m)
    for m in range(6):
        finish(m)


def gradients(x, dy, wg, wu, wd, bt=512):
    t, d = dy.shape
    ff = wg.shape[2]
    half = d // 2
    vmem = lambda *s: pltpu.VMEM(s, BF16)
    return pl.pallas_call(
        gradients_kernel,
        in_specs=[HBM] * 5,
        out_specs=[HBM] * 5,
        out_shape=[
            jax.ShapeDtypeStruct(s, BF16) for s in ((2, d, ff), (2, ff, half), (2, 2, half // 8, ff), (2, ff // 8, half), (ff, t))
        ],
        scratch_shapes=[
            vmem(2, d, ff),
            vmem(2, ff, half),
            vmem(2, d, ff),
            vmem(2, ff, half),
            vmem(4, half, ff),
            vmem(2, ff, half),
            vmem(4, 2, half // 4, ff),
            vmem(2, 2, ff // 4, half),
            vmem(4, 2, half // 8, ff),
            vmem(2, 2, ff // 8, half),
            vmem(ff, t),
            vmem(2, t, ff),
            vmem(d, t),
            vmem(t, d),
            vmem(t, d),
            vmem(t, d),
            vmem(d, 2 * ff),
            vmem(2, d, ff),
            vmem(2, ff, d),
            vmem(bt, ff),
            vmem(ff, bt),
            pltpu.SemaphoreType.DMA((9,)),
            pltpu.SemaphoreType.DMA,
            pltpu.SemaphoreType.DMA((3,)),
            pltpu.SemaphoreType.DMA((3, 2)),
            pltpu.SemaphoreType.DMA((6, 13)),
            pltpu.SemaphoreType.DMA((6, 13)),
            pltpu.SemaphoreType.REGULAR((3,)),
        ],
        compiler_params=pltpu.CompilerParams(collective_id=0, has_side_effects=True, vmem_limit_bytes=67043328),
        name="gradients",
    )(x, dy, wg, wu, wd)[:4]


def update_kernel(
    quarter_g, quarter_d, done_g, done_d, wg, wu, wd, mg, mu, md, vg, vu, vd,
    fg, fd, mg_out, mu_out, md_out, vg_out, vu_out, vd_out,
    own_g, own_d, load, quarters, send, recv,
):
    d, ff = wg.shape[1:]
    half = d // 2
    p = Places(d, ff)

    def f_ref(m, half, start, size):
        layer = ORDER[m][2]
        return p.share(m, fd.at[layer], fg.at[layer], half, start, size)

    def copy(m, kind, src, dst, device):
        at = (m - 3, kind - Y2)
        return pltpu.make_async_remote_copy(
            src_ref=src, dst_ref=dst, send_sem=send.at[at], recv_sem=recv.at[at], device_id={"dp": device}, device_id_type=MESH
        )

    def own_quarter(m, ab):
        q = p.height(m) // 8
        return p.core, p.sub_at(m, ab, p.keep[ab]) + p.quarter * q, q

    def summed(m, ab):
        return quarter_d.at[ab] if ORDER[m][0] else quarter_g.at[ORDER[m][1], ab]

    def y2(m, ab):
        ref = f_ref(m, *own_quarter(m, ab))
        return copy(m, Y2 + ab, ref, ref, p.far[ab])

    def mine(m, ab):
        return pltpu.make_async_copy(summed(m, ab), f_ref(m, *own_quarter(m, ab)), quarters.at[m - 3, ab])

    def y1(m, ab):
        ref = f_ref(m, p.core, p.sub_at(m, ab, p.keep[ab]), p.height(m) // 4)
        return copy(m, Y1 + ab, ref, ref, p.near[ab])

    def y0(m, ab):
        ref = f_ref(m, p.core, p.sub_at(m, ab, p.keep[ab]), p.height(m) // 4)
        return copy(m, Y0 + ab, ref, ref, p.other_core)

    def yr(m, ab):
        ref = f_ref(m, p.core, p.sub_at(m, ab, 1 - p.keep[ab]), p.height(m) // 4)
        return copy(m, YR + ab, ref, ref, p.other_core)

    def loads(m):
        is_down, i, layer = ORDER[m]
        w, mom, var = ((wd, md, vd), (wg, mg, vg), (wu, mu, vu))[0 if is_down else 1 + i]
        mom_out, var_out = ((md_out, vd_out), (mg_out, vg_out), (mu_out, vu_out))[0 if is_down else 1 + i]
        rest = [
            pltpu.make_async_copy(mom.at[layer], mom_out.at[layer], load.at[m, 1]),
            pltpu.make_async_copy(var.at[layer], var_out.at[layer], load.at[m, 2]),
        ]
        if layer:
            if is_down:
                rest.append(pltpu.make_async_copy(done_d, fd.at[layer], load.at[m, 3]))
            else:
                rest.append(pltpu.make_async_copy(done_g.at[i], fg.at[layer, i], load.at[m, 3]))
        to = own_d if is_down else own_g.at[i]
        return pltpu.make_async_copy(w.at[layer], to, load.at[m, 0]), rest

    def adamw(m, half_of, ab, which):
        is_down, i, layer = ORDER[m]
        mom, var = ((md_out, vd_out), (mg_out, vg_out), (mu_out, vu_out))[0 if is_down else 1 + i]
        size = p.height(m) // 4
        start = p.sub_at(m, ab, which)
        if is_down:
            at = (pl.ds(pl.multiple_of(start, 16), size), pl.ds(pl.multiple_of(half_of * half, half), half))
            w = own_d[at]
        else:
            at = (pl.ds(pl.multiple_of(half_of * half + start, 16), size), slice(None))
            w = own_g[(i, *at)]
        w = w.astype(F32)
        f = f_ref(m, half_of, start, size)
        g = f[...].astype(F32)
        new_m = 0.9 * mom[(layer, *at)] + 0.1 * g
        new_v = 0.95 * var[(layer, *at)] + 0.05 * g * g
        f[...] = (w - 0.02 * (new_m * lax.rsqrt(new_v + 1e-8) + 0.1 * w)).astype(BF16)
        mom[(layer, *at)] = new_m
        var[(layer, *at)] = new_v

    def c3(m):
        q = p.height(m) // 8
        for ab in range(2):
            y2(m, ab).wait_recv()
            y1(m, ab).start()
        for ab in range(2):
            y0(m, ab).start()

    def c4(m):
        for ab in range(2):
            y1(m, ab).wait_recv()
            yr(m, ab).start()

    def whole(m):
        own, rest = loads(m)
        own.wait()
        for c in rest:
            c.wait()

        def body(n, carry):
            adamw(m, n // 4, (n // 2) % 2, n % 2)
            return carry

        lax.fori_loop(0, 8, body, 0)
        loads(m + 3)[0].start()

    def others_kept(m):
        own, rest = loads(m)
        own.wait()
        for c in rest:
            c.wait()
        for ab in range(2):
            y0(m, ab).wait_recv()
            adamw(m, 1 - p.core, ab, p.keep[ab])

    def the_rest(m):
        for ab in range(2):
            y2(m, ab).wait_send()
            y0(m, ab).wait_send()
            y1(m, ab).wait_send()
            adamw(m, p.core, ab, p.keep[ab])
        for ab in range(2):
            yr(m, ab).wait_send()
            adamw(m, p.core, ab, 1 - p.keep[ab])
        for ab in range(2):
            yr(m, ab).wait_recv()
            adamw(m, 1 - p.core, ab, 1 - p.keep[ab])

    p.greet()
    for m in (3, 4, 5):
        for ab in range(2):
            mine(m, ab).start()
    for m in range(6):
        own, rest = loads(m)
        if m < 3:
            own.start()
        for c in rest:
            c.start()
    pl.semaphore_wait(pltpu.get_barrier_semaphore(), 3)
    for m in (3, 4, 5):
        for ab in range(2):
            mine(m, ab).wait()
            y2(m, ab).start()
    whole(0)
    c3(3)
    whole(1)
    c3(4)
    whole(2)
    c3(5)
    others_kept(3)
    c4(3)
    the_rest(3)
    others_kept(4)
    c4(4)
    the_rest(4)
    others_kept(5)
    c4(5)
    the_rest(5)


def update(weights, m, v, done_g, done_d, own_g, own_d):
    _, d, ff = weights[0].shape
    half = d // 2
    return pl.pallas_call(
        update_kernel,
        in_specs=[HBM] * 13,
        out_specs=[VMEM] * 8,
        out_shape=[pltpu.VMEM((2, 2, d, ff), BF16), pltpu.VMEM((2, 2, ff, half), BF16)] + [pltpu.VMEM(one.shape, F32) for one in (*m, *v)],
        scratch_shapes=[
            pltpu.VMEM((2, d, ff), BF16),
            pltpu.VMEM((ff, d), BF16),
            pltpu.SemaphoreType.DMA((6, 4)),
            pltpu.SemaphoreType.DMA((3, 2)),
            pltpu.SemaphoreType.DMA((3, 8)),
            pltpu.SemaphoreType.DMA((3, 8)),
        ],
        compiler_params=pltpu.CompilerParams(collective_id=1, has_side_effects=True, vmem_limit_bytes=12 * 2**20),
        name="update",
    )(own_g, own_d, done_g, done_d, *weights, *m, *v)


def written_kernel(fg, fd, mg, mu, md, vg, vu, vd, wg_out, wu_out, wd_out, mg_out, mu_out, md_out, vg_out, vu_out, vd_out, sem):
    layers, _, d, ff = fg.shape
    half = d // 2
    copies = [(one, to) for one, to in zip((mg, mu, md, vg, vu, vd), (mg_out, mu_out, md_out, vg_out, vu_out, vd_out), strict=True)]
    for l in range(layers):
        copies += [(fg.at[l, 0], wg_out.at[l]), (fg.at[l, 1], wu_out.at[l])]
        copies += [(fd.at[l, h], wd_out.at[l, :, pl.ds(h * half, half)]) for h in range(2)]
    copies = [pltpu.make_async_copy(a, b, sem.at[n]) for n, (a, b) in enumerate(copies)]
    for c in copies:
        c.start()
    for c in copies:
        c.wait()


def written(weights, values):
    return pl.pallas_call(
        written_kernel,
        in_specs=[VMEM] * 8,
        out_specs=[HBM] * 9,
        out_shape=[jax.ShapeDtypeStruct(w.shape, kind) for kind in (BF16, F32, F32) for w in weights],
        scratch_shapes=[pltpu.SemaphoreType.DMA((14,))],
        compiler_params=pltpu.CompilerParams(vmem_limit_bytes=12 * 2**20),
        name="written",
    )(*(pltpu.with_memory_space_constraint(one, pltpu.VMEM) for one in values))


def solution(mesh):
    def step(x, dy, *arrays):
        weights, m, v = (arrays[i : i + 3] for i in (0, 3, 6))
        summed = gradients(x[0], dy[0], *weights)
        return tuple(written(weights, update(weights, m, v, *summed)))

    return jax.shard_map(
        step,
        mesh=mesh,
        in_specs=(P(("rep", "dp"), None, None),) * 2 + (P(None, None, None),) * 9,
        out_specs=(P("rep", None, None),) * 9,
        check_vma=False,
    )
```

```python
import jax
import jax.numpy as jnp
from jax import lax
from jax.experimental import pallas as pl
from jax.experimental.pallas import tpu as pltpu
from jax.sharding import PartitionSpec as P

HBM = pl.BlockSpec(memory_space=pltpu.HBM)
VMEM = pl.BlockSpec(memory_space=pltpu.VMEM)
LANES = 128
BF16, F32 = jnp.bfloat16, jnp.float32
MESH = pl.DeviceIdType.MESH


def dot(a, b, dims=((1,), (0,))):
    return lax.dot_general(a, b, (dims, ((), ())), preferred_element_type=F32)


def dot_t(a, b):
    return dot(a, b, ((1,), (1,)))


def normed(h):
    wide = h.astype(F32)
    scale = lax.rsqrt(jnp.mean(wide * wide, -1, keepdims=True) + 1e-6)
    return (wide * scale).astype(BF16)


def interleaved(wg, wu, layer, to, sem):
    out = []
    for j in range(wg.shape[2] // LANES):
        for n, w in enumerate((wg, wu)):
            out.append(pltpu.make_async_copy(w.at[layer, :, pl.ds(j * LANES, LANES)], to.at[:, pl.ds((2 * j + n) * LANES, LANES)], sem))
    return out


def pairs(blocks):
    return [(at, min(2, blocks - at)) for at in range(0, blocks, 2)]


def backward_of_product(gate, up, dp):
    s = jax.nn.sigmoid(gate)
    silu = gate * s
    return silu, (dp * up * (s + silu * (1 - s))).astype(BF16), (dp * silu).astype(BF16)


ORDER = ((True, 0, 1), (False, 0, 1), (False, 1, 1), (True, 0, 0), (False, 0, 0), (False, 1, 0))
S0, X1, X2, Y2, Y1, Y0, YR = 0, 4, 6, 8, 10, 12, 14


class Places:
    def __init__(self, tokens_d, ff):
        self.d, self.ff = tokens_d, ff
        index = lax.axis_index("dp")
        self.core, chip = index % 2, index // 2
        chips = lax.axis_size("dp") // 2
        self.quarter = chip % 2
        after, before = (chip + 1) % chips, (chip + chips - 1) % chips
        first = jnp.where(self.quarter == 0, after, before)
        second = jnp.where(self.quarter == 0, before, after)
        self.other_core = chip * 2 + 1 - self.core
        self.near = (first * 2 + self.core, second * 2 + self.core)
        self.far = (self.near[1], self.near[0])
        self.keep = (((chip + 1) % chips) // 2, chip // 2)

    def height(self, m):
        return self.ff if ORDER[m][0] else self.d // 2

    def sub_at(self, m, ab, which):
        sub = self.height(m) // 4
        return (2 * ab + which) * sub

    def share(self, m, down, other, half, start, size):
        if ORDER[m][0]:
            return down.at[half, pl.ds(pl.multiple_of(start, 16), size), :]
        return other.at[ORDER[m][1], pl.ds(pl.multiple_of(half * (self.d // 2) + start, 16), size), :]

    def greet(self):
        barrier = pltpu.get_barrier_semaphore()
        for other in (self.other_core, *self.near):
            pl.semaphore_signal(barrier, inc=1, device_id={"dp": other}, device_id_type=MESH)


def part(ref, start, size):
    return ref.at[pl.ds(pl.multiple_of(start, 16), size), :]


def added(a, b):
    return (a[...].astype(F32) + b[...].astype(F32)).astype(BF16)


def gradients_kernel(
    x, dy, wg, wu, wd,
    done_g, done_d, own_g, own_d, mid0t,
    gg1, gd1, gg0, gd0, r0g, r0d, r1g, r1d, r2g, r2d,
    midt, dgu, at, av, dh, hv, wgu0, wgu1, wdv, midt_out,
    load, mid_store, store, quarters, send, recv, credit,
):
    t, d = dh.shape
    ff = wdv.shape[1]
    blocks = ff // LANES
    bt, fb = 256, midt_out.shape[1]
    half = d // 2
    p = Places(d, ff)

    def g_ref(m, half, start, size):
        return p.share(m, *((gd1, gg1) if ORDER[m][2] else (gd0, gg0)), half, start, size)

    def ref_of(m, down_ref, other_ref, *at):
        is_down, i, layer = ORDER[m]
        i = layer if is_down else 2 * layer + i
        return (down_ref if is_down else other_ref).at[(i, *at)]

    def copy(m, kind, src, dst, device):
        return pltpu.make_async_remote_copy(
            src_ref=src, dst_ref=dst, send_sem=send.at[m, kind], recv_sem=recv.at[m, kind], device_id={"dp": device}, device_id_type=MESH
        )

    def fourth(m, ab, kept):
        which = p.keep[ab] if kept else 1 - p.keep[ab]
        return p.sub_at(m, ab, which), p.height(m) // 4

    def s0(m, ab, kept):
        at = fourth(m, ab, kept)
        return copy(m, S0 + 2 * kept + ab, g_ref(m, 1 - p.core, *at), part(ref_of(m, r0d, r0g), *at), p.other_core)

    def x1(m, ab):
        src = part(ref_of(m, r0d, r0g), p.sub_at(m, ab, 1 - p.keep[ab]), p.height(m) // 4)
        return copy(m, X1 + ab, src, ref_of(m, r1d, r1g, ab), p.near[ab])

    def x2(m, ab):
        q = p.height(m) // 8
        return copy(m, X2 + ab, part(ref_of(m, r1d, r1g, ab), (1 - p.quarter) * q, q), ref_of(m, r2d, r2g, ab), p.far[ab])

    def y2(m, ab):
        q = p.height(m) // 8
        ref = g_ref(m, p.core, p.sub_at(m, ab, p.keep[ab]) + p.quarter * q, q)
        return copy(m, Y2 + ab, ref, ref, p.far[ab])

    def y1(m, ab):
        ref = g_ref(m, p.core, p.sub_at(m, ab, p.keep[ab]), p.height(m) // 4)
        return copy(m, Y1 + ab, ref, ref, p.near[ab])

    def y0(m):
        ref = g_ref(m, p.core, 0, p.height(m))
        return copy(m, Y0, ref, ref, p.other_core)

    def out(m):
        is_down, i, _ = ORDER[m]
        if is_down:
            return pltpu.make_async_copy(gd1, done_d, store.at[m])
        return pltpu.make_async_copy(gg1.at[i], done_g.at[i], store.at[m])

    def out_quarter(m, ab):
        to = own_d.at[ab] if ORDER[m][0] else own_g.at[ORDER[m][1], ab]
        return pltpu.make_async_copy(ref_of(m, r2d, r2g, ab), to, quarters.at[m - 3, ab])

    def pair_sum(m, ab, kept):
        s0(m, ab, kept).wait_recv()
        at = fourth(m, ab, kept)
        r0 = part(ref_of(m, r0d, r0g), *at)
        r0[...] = added(r0, g_ref(m, p.core, *at))

    def c0a(m):
        pair_sum(m, 0, 0)
        x1(m, 0).start()

    def c0b(m):
        pair_sum(m, 1, 0)
        x1(m, 1).start()

    def c0c(m):
        for ab in range(2):
            pair_sum(m, ab, 1)
        for ab in range(2):
            for kept in range(2):
                s0(m, ab, kept).wait_send()
        if ORDER[m][2]:
            pl.semaphore_signal(credit.at[m], inc=1, device_id={"dp": p.other_core}, device_id_type=MESH)

    def c0(m):
        c0a(m)
        c0b(m)
        c0c(m)

    def c1(m):
        for ab in range(2):
            x1(m, ab).wait_recv()
            r1 = ref_of(m, r1d, r1g, ab)
            r1[...] = added(r1, part(ref_of(m, r0d, r0g), p.sub_at(m, ab, p.keep[ab]), p.height(m) // 4))
            x2(m, ab).start()

    def c2(m):
        q = p.height(m) // 8
        for ab in range(2):
            x2(m, ab).wait_recv()
            if ORDER[m][2]:
                to = g_ref(m, p.core, p.sub_at(m, ab, p.keep[ab]) + p.quarter * q, q)
            else:
                to = ref_of(m, r2d, r2g, ab)
            to[...] = added(part(ref_of(m, r1d, r1g, ab), p.quarter * q, q), ref_of(m, r2d, r2g, ab))
            if ORDER[m][2]:
                y2(m, ab).start()
            else:
                out_quarter(m, ab).start()

    def c3(m):
        for ab in range(2):
            y2(m, ab).wait_recv()
            y1(m, ab).start()

    def c4(m):
        for ab in range(2):
            y1(m, ab).wait_recv()
        pl.semaphore_wait(credit.at[m], 1)
        y0(m).start()

    def c5(m):
        y0(m).wait_recv()
        out(m).start()

    def finish(m):
        for ab in range(2):
            for c in (x1, x2, y2, y1) if ORDER[m][2] else (x1, x2):
                c(m, ab).wait_send()
        if ORDER[m][2]:
            y0(m).wait_send()
            out(m).wait()
        else:
            for ab in range(2):
                out_quarter(m, ab).wait()

    def run(step, table):
        for when, todo in table.items():

            @pl.when(step == when)
            def _():
                for what, m in todo:
                    what(m)

    local = {
        "dy": pltpu.make_async_copy(dy, dh, load.at[0]),
        "wd0": pltpu.make_async_copy(wd.at[0], wdv.at[0], load.at[2]),
        "wg1": pltpu.make_async_copy(wg.at[1], wgu1.at[0], load.at[3]),
        "wu1": pltpu.make_async_copy(wu.at[1], wgu1.at[1], load.at[4]),
        "wd1": pltpu.make_async_copy(wd.at[1], wdv.at[1], load.at[5]),
        "mid0": pltpu.make_async_copy(mid0t, midt, load.at[6]),
    }
    xs = [pltpu.make_async_copy(x.at[pl.ds(i, n), :], hv.at[pl.ds(i, n), :], load.at[7 + k]) for k, (i, n) in enumerate(((0, fb), (fb, t - fb)))]
    xs[0].start()
    for c in interleaved(wg, wu, 0, wgu0, load.at[1]):
        c.start()
    local["wd0"].start()
    xs[1].start()
    for name in ("dy", "wd1", "wg1", "wu1"):
        local[name].start()
    p.greet()

    def middle_out(step):
        return pltpu.make_async_copy(midt_out, mid0t.at[:, pl.ds(pl.multiple_of(step * fb, fb), fb)], mid_store)

    def forward(step, carry):
        rows = pl.ds(pl.multiple_of(step * fb, fb), fb)

        @pl.when(step == 0)
        def _():
            xs[0].wait()
            pltpu.make_async_copy(wgu0, wgu0, load.at[1]).wait()

        @pl.when(step == 1)
        def _():
            xs[1].wait()

        @pl.when(step >= 1)
        def _():
            middle_out(step - 1).wait()

        h = hv[rows, :]
        a = normed(h)
        av[rows, :] = a
        for j in range(blocks):
            to = slice(j * LANES, (j + 1) * LANES)
            both = dot(a, wgu0[:, 2 * j * LANES : 2 * (j + 1) * LANES])
            gate, up = both[:, :LANES], both[:, LANES:]
            mid = (gate * jax.nn.sigmoid(gate) * up).astype(BF16)
            dgu[0, rows, to] = mid
            midt_out[to, :] = mid.T

        middle_out(step).start()

        @pl.when(step == 0)
        def _():
            for name in ("wd0", "dy", "wd1"):
                local[name].wait()

        h = h + dot(dgu[0, rows, :], wdv[0]).astype(BF16)
        by_h = dh[rows, :]
        for pair, width in pairs(blocks):
            to = slice(pair * LANES, (pair + width) * LANES)
            dgu[1, rows, to] = dot_t(by_h, wdv[1, to, :]).astype(BF16)
        hv[rows, :] = h
        a = normed(h)
        at[:, rows] = a.T

        @pl.when(step == 0)
        def _():
            for name in ("wg1", "wu1"):
                local[name].wait()

        for pair, width in pairs(blocks):
            to = slice(pair * LANES, (pair + width) * LANES)
            dp = dgu[1, rows, to].astype(F32)
            if width == 1:
                both = dot(a, jnp.concatenate([wgu1[0, :, to], wgu1[1, :, to]], 1))
                gate, up = both[:, :LANES], both[:, LANES:]
            else:
                gate, up = dot(a, wgu1[0, :, to]), dot(a, wgu1[1, :, to])
            silu, dg, du = backward_of_product(gate, up, dp)
            midt[to, rows] = (silu * up).astype(BF16).T
            dgu[0, rows, to], dgu[1, rows, to] = dg, du
        return carry

    lax.fori_loop(0, t // fb, forward, 0)
    middle_out(t // fb - 1).wait()

    def down_grad(m, gd, table, steps=(0, 8)):
        sub = ff // 4

        def body(step, carry):
            kept, own, ab = step // 4, (step % 4) // 2, step % 2
            which = jnp.where(own == 0, 1 - p.core, p.core)
            keep = jnp.where(ab == 0, p.keep[0], p.keep[1])
            at = 2 * ab + jnp.where(kept == 0, 1 - keep, keep)
            rows = pl.ds(pl.multiple_of(at * sub, 16), sub)
            gd[which, rows, :] = dot(midt[rows, :], dh[:, pl.ds(pl.multiple_of(which * half, half), half)]).astype(BF16)
            for k in range(2):
                for n in range(2):

                    @pl.when(step == 4 * k + n)
                    def _():
                        s0(m, n, k).start()

            run(step, table)
            return carry

        lax.fori_loop(*steps, body, 0)

    def other_grads(m, gg, table, steps=(0, 4)):
        def body(step, carry):
            which = jnp.where(step % 2 == 0, 1 - p.core, p.core)
            rows = pl.ds(pl.multiple_of(which * half, half), half)
            gg[step // 2, rows, :] = dot(at[rows, :], dgu[step // 2]).astype(BF16)
            for n in range(2):

                @pl.when(step == 2 * n)
                def _():
                    for kept in range(2):
                        for ab in range(2):
                            s0(m + n, ab, kept).start()

            run(step, table)
            return carry

        lax.fori_loop(*steps, body, 0)

    pl.semaphore_wait(pltpu.get_barrier_semaphore(), 3)
    down_grad(0, gd1, {3: [(c0a, 0), (c0b, 0)]}, (0, 4))
    other_grads(1, gg1, {1: [(c0a, 1), (c0b, 1)]}, (0, 2))
    down_grad(0, gd1, {}, (4, 8))
    local["mid0"].start()
    other_grads(1, gg1, {2: [(c0c, 0), (c0c, 1), (c1, 0)], 3: [(c0, 2)]}, (2, 4))

    def states_grad(step, carry):
        rows = pl.ds(pl.multiple_of(step * bt, bt), bt)
        by_a = dot_t(dgu[0, rows, :], wgu1[0]).astype(BF16) + dot_t(dgu[1, rows, :], wgu1[1]).astype(BF16)
        by_a = by_a.astype(F32)
        wide = hv[rows, :].astype(F32)
        scale = lax.rsqrt(jnp.mean(wide * wide, -1, keepdims=True) + 1e-6)
        along = jnp.mean(by_a * wide, -1, keepdims=True) * (scale * scale * scale)
        dh[rows, :] = dh[rows, :] + (by_a * scale - wide * along).astype(BF16)
        run(step, {0: [(c1, 1)], 2: [(c2, 0)], 6: [(c1, 2)]})
        return carry

    lax.fori_loop(0, t // bt, states_grad, 0)

    local["mid0"].wait()
    down_grad(3, gd0, {0: [(c2, 1)], 3: [(c3, 0), (c0a, 3)], 4: [(c0b, 3)]})

    def layer_back(step, carry):
        rows = pl.ds(pl.multiple_of(step * bt, bt), bt)
        a, by_h = av[rows, :], dh[rows, :]
        at[:, rows] = a.T
        for pair, width in pairs(blocks):
            dp2 = dot_t(by_h, wdv[0, pair * LANES : (pair + width) * LANES, :]).astype(BF16).astype(F32)
            for j in range(pair, pair + width):
                to = slice(j * LANES, (j + 1) * LANES)
                both = dot(a, wgu0[:, 2 * j * LANES : 2 * (j + 1) * LANES])
                _, dg, du = backward_of_product(both[:, :LANES], both[:, LANES:], dp2[:, (j - pair) * LANES : (j - pair + 1) * LANES])
                dgu[0, rows, to], dgu[1, rows, to] = dg, du
        run(step, {0: [(c0c, 3), (c2, 2)], 1: [(c3, 1)], 3: [(c4, 0)], 5: [(c5, 0)], 6: [(c1, 3)], 7: [(c3, 2)]})
        return carry

    lax.fori_loop(0, t // bt, layer_back, 0)
    other_grads(4, gg0, {1: [(c0, 4), (c4, 1)], 3: [(c0, 5), (c2, 3), (c5, 1)]})
    for what, m in [(c4, 2), (c1, 4), (c5, 2), (c1, 5), (c2, 4), (c2, 5)]:
        what(m)
    for m in range(6):
        finish(m)


def gradients(x, dy, wg, wu, wd, bt=1024):
    t, d = dy.shape
    ff = wg.shape[2]
    half = d // 2
    vmem = lambda *s: pltpu.VMEM(s, BF16)
    return pl.pallas_call(
        gradients_kernel,
        in_specs=[HBM] * 5,
        out_specs=[HBM] * 5,
        out_shape=[
            jax.ShapeDtypeStruct(s, BF16) for s in ((2, d, ff), (2, ff, half), (2, 2, half // 8, ff), (2, ff // 8, half), (ff, t))
        ],
        scratch_shapes=[
            vmem(2, d, ff),
            vmem(2, ff, half),
            vmem(2, d, ff),
            vmem(2, ff, half),
            vmem(4, half, ff),
            vmem(2, ff, half),
            vmem(4, 2, half // 4, ff),
            vmem(2, 2, ff // 4, half),
            vmem(4, 2, half // 8, ff),
            vmem(2, 2, ff // 8, half),
            vmem(ff, t),
            vmem(2, t, ff),
            vmem(d, t),
            vmem(t, d),
            vmem(t, d),
            vmem(t, d),
            vmem(d, 2 * ff),
            vmem(2, d, ff),
            vmem(2, ff, d),
            vmem(ff, bt),
            pltpu.SemaphoreType.DMA((9,)),
            pltpu.SemaphoreType.DMA,
            pltpu.SemaphoreType.DMA((3,)),
            pltpu.SemaphoreType.DMA((3, 2)),
            pltpu.SemaphoreType.DMA((6, 13)),
            pltpu.SemaphoreType.DMA((6, 13)),
            pltpu.SemaphoreType.REGULAR((3,)),
        ],
        compiler_params=pltpu.CompilerParams(collective_id=0, has_side_effects=True, vmem_limit_bytes=67043328),
        name="gradients",
    )(x, dy, wg, wu, wd)[:4]


def update_kernel(
    quarter_g, quarter_d, done_g, done_d, wg, wu, wd, mg, mu, md, vg, vu, vd,
    fg, fd, mg_out, mu_out, md_out, vg_out, vu_out, vd_out,
    own_g, own_d, load, quarters, send, recv,
):
    d, ff = wg.shape[1:]
    half = d // 2
    p = Places(d, ff)

    def f_ref(m, half, start, size):
        layer = ORDER[m][2]
        return p.share(m, fd.at[layer], fg.at[layer], half, start, size)

    def copy(m, kind, src, dst, device):
        at = (m - 3, kind - Y2)
        return pltpu.make_async_remote_copy(
            src_ref=src, dst_ref=dst, send_sem=send.at[at], recv_sem=recv.at[at], device_id={"dp": device}, device_id_type=MESH
        )

    def own_quarter(m, ab):
        q = p.height(m) // 8
        return p.core, p.sub_at(m, ab, p.keep[ab]) + p.quarter * q, q

    def summed(m, ab):
        return quarter_d.at[ab] if ORDER[m][0] else quarter_g.at[ORDER[m][1], ab]

    def y2(m, ab):
        ref = f_ref(m, *own_quarter(m, ab))
        return copy(m, Y2 + ab, ref, ref, p.far[ab])

    def mine(m, ab):
        return pltpu.make_async_copy(summed(m, ab), f_ref(m, *own_quarter(m, ab)), quarters.at[m - 3, ab])

    def y1(m, ab):
        ref = f_ref(m, p.core, p.sub_at(m, ab, p.keep[ab]), p.height(m) // 4)
        return copy(m, Y1 + ab, ref, ref, p.near[ab])

    def y0(m, ab):
        ref = f_ref(m, p.core, p.sub_at(m, ab, p.keep[ab]), p.height(m) // 4)
        return copy(m, Y0 + ab, ref, ref, p.other_core)

    def yr(m, ab):
        ref = f_ref(m, p.core, p.sub_at(m, ab, 1 - p.keep[ab]), p.height(m) // 4)
        return copy(m, YR + ab, ref, ref, p.other_core)

    def loads(m):
        is_down, i, layer = ORDER[m]
        w, mom, var = ((wd, md, vd), (wg, mg, vg), (wu, mu, vu))[0 if is_down else 1 + i]
        mom_out, var_out = ((md_out, vd_out), (mg_out, vg_out), (mu_out, vu_out))[0 if is_down else 1 + i]
        rest = [
            pltpu.make_async_copy(mom.at[layer], mom_out.at[layer], load.at[m, 1]),
            pltpu.make_async_copy(var.at[layer], var_out.at[layer], load.at[m, 2]),
        ]
        if layer:
            if is_down:
                rest.append(pltpu.make_async_copy(done_d, fd.at[layer], load.at[m, 3]))
            else:
                rest.append(pltpu.make_async_copy(done_g.at[i], fg.at[layer, i], load.at[m, 3]))
        to = own_d if is_down else own_g.at[i]
        return pltpu.make_async_copy(w.at[layer], to, load.at[m, 0]), rest

    def adamw(m, half_of, ab, which):
        is_down, i, layer = ORDER[m]
        mom, var = ((md_out, vd_out), (mg_out, vg_out), (mu_out, vu_out))[0 if is_down else 1 + i]
        size = p.height(m) // 4
        start = p.sub_at(m, ab, which)
        if is_down:
            at = (pl.ds(pl.multiple_of(start, 16), size), pl.ds(pl.multiple_of(half_of * half, half), half))
            w = own_d[at]
        else:
            at = (pl.ds(pl.multiple_of(half_of * half + start, 16), size), slice(None))
            w = own_g[(i, *at)]
        w = w.astype(F32)
        f = f_ref(m, half_of, start, size)
        g = f[...].astype(F32)
        new_m = 0.9 * mom[(layer, *at)] + 0.1 * g
        new_v = 0.95 * var[(layer, *at)] + 0.05 * g * g
        f[...] = (w - 0.02 * (new_m * lax.rsqrt(new_v + 1e-8) + 0.1 * w)).astype(BF16)
        mom[(layer, *at)] = new_m
        var[(layer, *at)] = new_v

    def c3(m):
        q = p.height(m) // 8
        for ab in range(2):
            y2(m, ab).wait_recv()
            y1(m, ab).start()
        for ab in range(2):
            y0(m, ab).start()

    def c4(m):
        for ab in range(2):
            y1(m, ab).wait_recv()
            yr(m, ab).start()

    def whole(m):
        own, rest = loads(m)
        own.wait()
        for c in rest:
            c.wait()

        def body(n, carry):
            adamw(m, n // 4, (n // 2) % 2, n % 2)
            return carry

        lax.fori_loop(0, 8, body, 0)
        loads(m + 3)[0].start()

    def others_kept(m):
        own, rest = loads(m)
        own.wait()
        for c in rest:
            c.wait()
        for ab in range(2):
            y0(m, ab).wait_recv()
            adamw(m, 1 - p.core, ab, p.keep[ab])

    def the_rest(m):
        for ab in range(2):
            y2(m, ab).wait_send()
            y0(m, ab).wait_send()
            y1(m, ab).wait_send()
            adamw(m, p.core, ab, p.keep[ab])
        for ab in range(2):
            yr(m, ab).wait_send()
            adamw(m, p.core, ab, 1 - p.keep[ab])
        for ab in range(2):
            yr(m, ab).wait_recv()
            adamw(m, 1 - p.core, ab, 1 - p.keep[ab])

    p.greet()
    for m in (3, 4, 5):
        for ab in range(2):
            mine(m, ab).start()
    pl.semaphore_wait(pltpu.get_barrier_semaphore(), 3)
    for m in (3, 4, 5):
        for ab in range(2):
            mine(m, ab).wait()
            y2(m, ab).start()
    for m in range(6):
        own, rest = loads(m)
        if m < 3:
            own.start()
        for c in rest:
            c.start()
    whole(0)
    c3(3)
    whole(1)
    c3(4)
    whole(2)
    c3(5)
    others_kept(3)
    c4(3)
    the_rest(3)
    others_kept(4)
    c4(4)
    the_rest(4)
    others_kept(5)
    c4(5)
    the_rest(5)


def update(weights, m, v, done_g, done_d, own_g, own_d):
    _, d, ff = weights[0].shape
    half = d // 2
    return pl.pallas_call(
        update_kernel,
        in_specs=[HBM] * 13,
        out_specs=[VMEM] * 8,
        out_shape=[pltpu.VMEM((2, 2, d, ff), BF16), pltpu.VMEM((2, 2, ff, half), BF16)] + [pltpu.VMEM(one.shape, F32) for one in (*m, *v)],
        scratch_shapes=[
            pltpu.VMEM((2, d, ff), BF16),
            pltpu.VMEM((ff, d), BF16),
            pltpu.SemaphoreType.DMA((6, 4)),
            pltpu.SemaphoreType.DMA((3, 2)),
            pltpu.SemaphoreType.DMA((3, 8)),
            pltpu.SemaphoreType.DMA((3, 8)),
        ],
        compiler_params=pltpu.CompilerParams(collective_id=1, has_side_effects=True, vmem_limit_bytes=12 * 2**20),
        name="update",
    )(own_g, own_d, done_g, done_d, *weights, *m, *v)


def written_kernel(fg, fd, mg, mu, md, vg, vu, vd, wg_out, wu_out, wd_out, mg_out, mu_out, md_out, vg_out, vu_out, vd_out, sem):
    layers, _, d, ff = fg.shape
    half = d // 2
    copies = [(one, to) for one, to in zip((mg, mu, md, vg, vu, vd), (mg_out, mu_out, md_out, vg_out, vu_out, vd_out), strict=True)]
    for l in range(layers):
        copies += [(fg.at[l, 0], wg_out.at[l]), (fg.at[l, 1], wu_out.at[l])]
        copies += [(fd.at[l, h], wd_out.at[l, :, pl.ds(h * half, half)]) for h in range(2)]
    copies = [pltpu.make_async_copy(a, b, sem.at[n]) for n, (a, b) in enumerate(copies)]
    for c in copies:
        c.start()
    for c in copies:
        c.wait()


def written(weights, values):
    return pl.pallas_call(
        written_kernel,
        in_specs=[VMEM] * 8,
        out_specs=[HBM] * 9,
        out_shape=[jax.ShapeDtypeStruct(w.shape, kind) for kind in (BF16, F32, F32) for w in weights],
        scratch_shapes=[pltpu.SemaphoreType.DMA((14,))],
        compiler_params=pltpu.CompilerParams(vmem_limit_bytes=12 * 2**20),
        name="written",
    )(*(pltpu.with_memory_space_constraint(one, pltpu.VMEM) for one in values))


def solution(mesh):
    def step(x, dy, *arrays):
        weights, m, v = (arrays[i : i + 3] for i in (0, 3, 6))
        summed = gradients(x[0], dy[0], *weights)
        return tuple(written(weights, update(weights, m, v, *summed)))

    return jax.shard_map(
        step,
        mesh=mesh,
        in_specs=(P(("rep", "dp"), None, None),) * 2 + (P(None, None, None),) * 9,
        out_specs=(P("rep", None, None),) * 9,
        check_vma=False,
    )
```
